128 devices in a mesh: rep: 1, r: 16 (over y, z), s: 8 (over x, core).
Axes of the slice: x: 4, y: 4, z: 4, core: 2. Of those that a mesh axis runs over, the one named last changes fastest.
Arguments:
- x: bfloat16 [128, 2048, 640], P(('rep', 'r', 's'))
- dy: bfloat16 [128, 2048, 640], P(('rep', 'r', 's'))
- w_gate: bfloat16 [2, 640, 4096], P(None, 's')
- w_up: bfloat16 [2, 640, 4096], P(None, 's')
- w_down: bfloat16 [2, 4096, 640], P(None, 's')
Outputs:
- output 1: bfloat16 [128, 2048, 640], P(('rep', 'r', 's'))
- output 2: bfloat16 [2, 640, 4096], P('rep', 's')
- output 3: bfloat16 [2, 640, 4096], P('rep', 's')
- output 4: bfloat16 [2, 4096, 640], P('rep', 's')
All inputs are finite; a program needn't handle non-finite values.
Results may differ from the reference program's by a relative error of at most 0.018.
Values are sent between devices in bfloat16 or wider.
A program may use at most 1.5 GiB of HBM per device.

```python
import jax
import jax.numpy as jnp
from jax import lax

SEQUENCES = 128
TOKENS = 2048
D = 640
FF = 4096
LAYERS = 2
NAMES = ("w_gate", "w_up", "w_down")
SHAPES = {"w_gate": (LAYERS, D, FF), "w_up": (LAYERS, D, FF), "w_down": (LAYERS, FF, D)}


def bump(key, n, height):
    away = (jnp.arange(n, dtype=jnp.int32) - jax.random.randint(key, (), 0, n, jnp.int32)) % n
    return jnp.where(away < n // 8, height, 1.0)


def together(key, own, strength):
    shared = jax.random.normal(key, own.shape[1:], jnp.float32)
    return (own + strength * shared) * lax.rsqrt(1 + strength * strength)


def setup_inputs(seed: int = 0, part: int = 0) -> dict:
    kx, kdy, ka, kb, kz, kf, kh, kl, *kw = jax.random.split(jax.random.key(seed), 8 + len(NAMES))
    kx, kdy, ka, kb = (jax.random.fold_in(k, part) for k in (kx, kdy, ka, kb))
    shape = (SEQUENCES, TOKENS, D)
    much_x, much_dy = jax.random.uniform(kz, (2,), jnp.float32, 0.0, 1.0)
    layers = 2.0 ** jax.random.uniform(kl, (LAYERS, 1, 1), jnp.float32, -1.0, 1.0)
    x = together(ka, jax.random.normal(kx, shape, jnp.float32), much_x) * bump(kf, D, 4.0)
    dy = together(kb, jax.random.normal(kdy, shape, jnp.float32), much_dy)
    drawn = {"x": x.astype(jnp.bfloat16), "dy": (dy * (SEQUENCES * TOKENS) ** -0.5).astype(jnp.bfloat16)}
    for key, name in zip(kw, NAMES, strict=True):
        w = jax.random.normal(key, SHAPES[name], jnp.float32) * SHAPES[name][1] ** -0.5
        drawn[name] = (w * {"w_gate": 1.0, "w_up": bump(kh, FF, 4.0), "w_down": layers}[name]).astype(jnp.bfloat16)
    return drawn


def matmul(a, w):
    return jnp.dot(a, w, preferred_element_type=jnp.float32).astype(jnp.bfloat16)


def normed(h):
    wide = h.astype(jnp.float32)
    scale = lax.rsqrt(jnp.mean(wide**2, -1, keepdims=True) + 1e-6)
    return (wide * scale).astype(jnp.bfloat16)


def layer(h, w):
    a = normed(h)
    gate = jnp.dot(a, w["w_gate"], preferred_element_type=jnp.float32)
    up = jnp.dot(a, w["w_up"], preferred_element_type=jnp.float32)
    return h + matmul((jax.nn.silu(gate) * up).astype(jnp.bfloat16), w["w_down"])


def stack(weights, h):
    return lax.scan(lambda h, w: (layer(h, w), None), h, weights)[0]


def reference(x, dy, w_gate, w_up, w_down):
    weights = dict(zip(NAMES, (w_gate, w_up, w_down), strict=True))

    def take(so_far, sequence):
        h, by_y = sequence
        _, back = jax.vjp(stack, weights, h)
        by_weights, by_h = back(by_y)
        return jax.tree.map(lambda total, term: total + term.astype(jnp.float32), so_far, by_weights), by_h

    none_yet = {name: jnp.zeros(w.shape, jnp.float32) for name, w in weights.items()}
    by_weights, by_x = lax.scan(take, none_yet, (x, dy))
    return (by_x, *(by_weights[name].astype(jnp.bfloat16) for name in NAMES))
```

```python
import functools

import jax
import jax.numpy as jnp
from jax import lax
from jax.experimental import pallas as pl
from jax.experimental.pallas import tpu as pltpu
from jax.sharding import PartitionSpec as P

NAMES = ("w_gate", "w_up", "w_down")
F32, BF16 = jnp.float32, jnp.bfloat16


def matmul(a, w):
    return jnp.dot(a, w, preferred_element_type=jnp.float32).astype(jnp.bfloat16)


def normed(h):
    wide = h.astype(jnp.float32)
    scale = lax.rsqrt(jnp.mean(wide**2, -1, keepdims=True) + 1e-6)
    return (wide * scale).astype(jnp.bfloat16)


def layer(h, w):
    a = normed(h)
    gate = jnp.dot(a, w["w_gate"], preferred_element_type=jnp.float32)
    up = jnp.dot(a, w["w_up"], preferred_element_type=jnp.float32)
    return h + matmul((jax.nn.silu(gate) * up).astype(jnp.bfloat16), w["w_down"])


class Place:
    def __init__(self):
        s, r = lax.axis_index("s"), lax.axis_index("r")
        self.rep = lax.axis_index("rep")
        self.x, self.c, self.y, self.z = s // 2, s % 2, r // 4, r % 4
        self.at = {"x": self.x, "y": self.y, "z": self.z}

    def device(self, axis=None, by=0):
        at = dict(self.at)
        c = self.c
        if axis is None:
            c = 1 - c
        else:
            at[axis] = (at[axis] + by) % 4
        return (self.rep, at["y"] * 4 + at["z"], at["x"] * 2 + c)

    def barrier(self):
        semaphore = pltpu.get_barrier_semaphore()
        for who in [self.device()] + [self.device(a, by) for a in "xyz" for by in (1, 3)]:
            pl.semaphore_signal(semaphore, inc=1, device_id=who, device_id_type=pl.DeviceIdType.MESH)
        pl.semaphore_wait(semaphore, 7)


class Sender:
    def __init__(self, send, recv):
        self.send, self.recv, self.n, self.started = send, recv, 0, []

    def copy(self, src, dst, who):
        k, self.n = self.n, self.n + 1
        made = pltpu.make_async_remote_copy(
            src_ref=src,
            dst_ref=dst,
            send_sem=self.send.at[k],
            recv_sem=self.recv.at[k],
            device_id=who,
            device_id_type=pl.DeviceIdType.MESH,
        )
        made.start()
        self.started.append(made)
        return made

    def finish(self):
        for made in self.started:
            made.wait_send()


class Part:
    def __init__(self, own, out, axis, dim, base, size):
        self.own, self.out, self.axis, self.dim, self.base, self.size = own, out, axis, dim, base, size

    def cut(self, q, half):
        w = self.size // 4
        start = self.base + q * w
        if half is not None:
            w //= 2
            start = start + half * w
        if isinstance(start, int):
            return pl.ds(start, w)
        return pl.ds(pl.multiple_of(start, w), w)

    def mine(self, q, half=None):
        d = self.cut(q, half)
        return self.own.at[:, d] if self.dim else self.own.at[d]

    def there(self, x, c, q, half=None):
        d = self.cut(q, half)
        return self.out.at[x, c, :, d] if self.dim else self.out.at[x, c, d]


GATHER_COPIES = 3 + 4 * 32


def gather_kernel(g, u, d, og, ou, od, send, recv, local):
    me = Place()
    x, c = me.x, me.c
    here = []
    for i, (own, out) in enumerate(((g, og), (u, ou), (d, od))):
        here.append(pltpu.make_async_copy(own, out.at[x, c], local.at[i]))
        here[-1].start()
    me.barrier()
    go = Sender(send, recv)
    other = me.device()
    columns, rows = g.shape[1], d.shape[0]
    parts = [
        Part(g, og, "y", 1, 0, columns // 2),
        Part(g, og, "z", 1, columns // 2, columns // 2),
        Part(u, ou, "y", 1, 0, columns),
        Part(d, od, "z", 0, 0, rows),
    ]
    x1, x2, x3 = (x + 1) % 4, (x + 2) % 4, (x + 3) % 4
    across = []
    first = []
    for p in parts:
        q = me.at[p.axis]
        first.append(
            (
                go.copy(p.mine(q), p.there(x, c, q), me.device("x", 1)),
                go.copy(p.mine(q), p.there(x, c, q), me.device("x", 3)),
            )
        )
    for own, out in ((g, og), (u, ou), (d, od)):
        across.append(go.copy(own, out.at[x, c], other))
    second, along = [], []
    for p, (left, right) in zip(parts, first):
        q = me.at[p.axis]
        up, down = me.device(p.axis, 1), me.device(p.axis, 3)
        left.wait_recv()
        a = go.copy(p.there(x3, c, q, 0), p.there(x3, c, q, 0), me.device("x", 1))
        l = [go.copy(p.there(x3, c, q), p.there(x3, c, q), who) for who in (up, down)]
        across.append(go.copy(p.there(x3, c, q), p.there(x3, c, q), other))
        right.wait_recv()
        b = go.copy(p.there(x1, c, q, 1), p.there(x1, c, q, 1), me.device("x", 3))
        r = [go.copy(p.there(x1, c, q), p.there(x1, c, q), who) for who in (up, down)]
        across.append(go.copy(p.there(x1, c, q), p.there(x1, c, q), other))
        second.append((a, b))
        along.append([(x3, l), (x1, r)])
    for p, (a, b), l in zip(parts, second, along):
        q = me.at[p.axis]
        up, down = me.device(p.axis, 1), me.device(p.axis, 3)
        a.wait_recv()
        b.wait_recv()
        l.append((x2, [go.copy(p.there(x2, c, q), p.there(x2, c, q), who) for who in (up, down)]))
        across.append(go.copy(p.there(x2, c, q), p.there(x2, c, q), other))
    last = []
    for k in range(3):
        for p, l in zip(parts, along):
            q = me.at[p.axis]
            q1, q3 = (q + 1) % 4, (q + 3) % 4
            up, down = me.device(p.axis, 1), me.device(p.axis, 3)
            at, (below, above) = l[k]
            below.wait_recv()
            last.append((p, at, 0, go.copy(p.there(at, c, q3, 0), p.there(at, c, q3, 0), up)))
            across.append(go.copy(p.there(at, c, q3), p.there(at, c, q3), other))
            above.wait_recv()
            last.append((p, at, 1, go.copy(p.there(at, c, q1, 1), p.there(at, c, q1, 1), down)))
            across.append(go.copy(p.there(at, c, q1), p.there(at, c, q1), other))
    for p, at, half, made in last:
        q2 = (me.at[p.axis] + 2) % 4
        made.wait_recv()
        across.append(go.copy(p.there(at, c, q2, half), p.there(at, c, q2, half), other))
    for made in across:
        made.wait_recv()
    for made in here:
        made.wait()
    go.finish()


def gathered(g, u, d):
    vmem, hbm = pl.BlockSpec(memory_space=pltpu.VMEM), pl.BlockSpec(memory_space=pltpu.HBM)
    out = pl.pallas_call(
        gather_kernel,
        out_shape=[jax.ShapeDtypeStruct((4, 2, *w.shape), w.dtype) for w in (g, u, d)],
        in_specs=[vmem] * 3,
        out_specs=[hbm] * 3,
        scratch_shapes=[
            pltpu.SemaphoreType.DMA((GATHER_COPIES,)),
            pltpu.SemaphoreType.DMA((GATHER_COPIES,)),
            pltpu.SemaphoreType.DMA((3,)),
        ],
        compiler_params=pltpu.CompilerParams(collective_id=0, has_side_effects=True),
        name="gather_weights",
    )(g, u, d)
    return [o.reshape(8 * o.shape[2], o.shape[3]) for o in out]


def added(dst, *srcs):
    shape = dst.shape
    if len(shape) == 3:
        for i in range(shape[0]):
            added(dst.at[i], *(s.at[i] for s in srcs))
        return
    rows, columns = shape
    step = 16 if rows % 16 == 0 else rows
    wide = min(columns, 1024)

    @pl.loop(0, rows // step)
    def _(i):
        for j in range(0, columns, wide):
            at = (pl.ds(pl.multiple_of(i * step, step), step), pl.ds(j, min(wide, columns - j)))
            total = srcs[0][at].astype(F32)
            for s in srcs[1:]:
                total = total + s[at].astype(F32)
            dst[at] = total.astype(dst.dtype)


class Ring:
    def __init__(self, me, go, axis, terms, cut, out, got, hold):
        self.me, self.go, self.terms, self.cut, self.out, self.got, self.hold = me, go, terms, cut, out, got, hold
        self.p = me.at[axis]
        self.up, self.down = me.device(axis, 1), me.device(axis, 3)

    def term(self, k, half):
        return [self.cut(t, (self.p + k) % 4, half) for t in self.terms]

    def send(self, slot, k, half, who, *more):
        held = self.hold.at[slot]
        added(held, *self.term(k, half), *more)
        return self.go.copy(held, self.got.at[slot], who)

    def start(self):
        self.far = (self.send(0, 2, 0, self.up), self.send(1, 2, 1, self.down))
        self.near = [self.send(2, 1, 1, self.up), self.send(3, 3, 0, self.down)]

    def middle(self):
        self.far[0].wait_recv()
        self.near.append(self.send(4, 1, 0, self.up, self.got.at[0]))
        self.far[1].wait_recv()
        self.near.append(self.send(5, 3, 1, self.down, self.got.at[1]))

    def end(self, cut_out):
        for made in self.near:
            made.wait_recv()
        added(cut_out(self.out, 0), *self.term(0, 0), self.got.at[3], self.got.at[4])
        added(cut_out(self.out, 1), *self.term(0, 1), self.got.at[2], self.got.at[5])


def piece(dim, n):
    def cut(ref, q, half):
        w = ref.shape[dim] // 4
        at = [slice(None)] * len(ref.shape)
        if n == dim:
            at[dim] = pl.ds(pl.multiple_of(q * w + half * (w // 2), w // 2), w // 2)
        else:
            at[dim] = pl.ds(pl.multiple_of(q * w, w), w)
            h = ref.shape[n] // 2
            at[n] = pl.ds(half * h, h)
        if dim == 0 and len(ref.shape) == 3:
            at[0] = q
        return ref.at[tuple(at)]

    return cut


def halves(n):
    def cut(ref, half):
        h = ref.shape[n] // 2
        at = [slice(None)] * len(ref.shape)
        at[n] = pl.ds(half * h, h)
        return ref.at[tuple(at)]

    return cut


ROUTES = (
    (1, (("x", 0, 2), ("y", 1, 1), ("z", 1, 1))),
    (1, (("y", 2, 0), ("z", 2, 0), ("x", 0, 2))),
    (0, (("z", 1, 0), ("x", 0, 1), ("y", 0, 0))),
)


def plan(shape, steps):
    sizes = []
    for _, dim, n in steps:
        cut = list(shape)
        if dim == 0 and len(cut) == 3:
            cut = cut[1:]
            whole = list(cut)
            cut[n - 1] //= 2
        else:
            cut[dim] //= 4
            whole = list(cut)
            cut[n] //= 2
        sizes.append((tuple(cut), tuple(whole)))
        shape = tuple(whole)
    return sizes


REDUCE_COPIES = 3 * (1 + 18 + 3 + 4)


def reduce_kernel(*refs):
    terms, outs, scratch = refs[:3], refs[3:6], list(refs[6:])
    send, recv, local = scratch[-3:]
    per = (len(scratch) - 3) // 3
    me = Place()
    c = me.c
    here = []
    for m in range(3):
        own = scratch[m * per]
        here.append(pltpu.make_async_copy(terms[m].at[:, c], own, local.at[m]))
        here[-1].start()
    me.barrier()
    go = Sender(send, recv)
    other = me.device()
    swaps = [go.copy(terms[m].at[:, 1 - c], scratch[m * per + 1], other) for m in range(3)]
    rings = [None] * 3
    for m in range(3):
        b = scratch[m * per : (m + 1) * per]
        axis, dim, n = ROUTES[m][1][0]
        here[m].wait()
        swaps[m].wait_recv()
        rings[m] = Ring(me, go, axis, (b[0], b[1]), piece(dim, n), b[2], b[3], b[4])
        rings[m].start()
    for step in range(3):
        for m in range(3):
            rings[m].middle()
        for m in range(3):
            b = scratch[m * per : (m + 1) * per]
            axis, dim, n = ROUTES[m][1][step]
            drop = dim == 0 and len(rings[m].terms[0].shape) == 3
            rings[m].end(halves(n - 1 if drop else n))
            if step < 2:
                axis, dim, n = ROUTES[m][1][step + 1]
                nxt = b[2 + 3 * (step + 1) :]
                rings[m] = Ring(me, go, axis, (b[2 + 3 * step],), piece(dim, n), nxt[0], nxt[1], nxt[2])
                rings[m].start()
    state = []
    for m in range(3):
        dim = ROUTES[m][0]
        b = scratch[m * per : (m + 1) * per]
        total, done = b[8], b[11]
        high, low = ("z", "y") if m == 2 else ("y", "z")
        size = done.shape[dim] // 16

        def at(hi, lo=None, half=None, done=done, dim=dim, size=size):
            w = size if lo is not None else 4 * size
            start = hi * (4 * size) + (lo * size if lo is not None else 0)
            if half is not None:
                w //= 2
                start = start + half * w
            d = pl.ds(pl.multiple_of(start, w), w)
            return done.at[:, d] if dim else done.at[d]

        h, l = me.at[high], me.at[low]
        added(at(h, l), total)
        made = [go.copy(at(h, l), at(h, l), me.device(low, k)) for k in (1, 2, 3)]
        state.append((at, high, h, made))
    near = []
    for at, high, h, made in state:
        for k in made:
            k.wait_recv()
        near.append((go.copy(at(h), at(h), me.device(high, 1)), go.copy(at(h), at(h), me.device(high, 3))))
    last = []
    for (at, high, h, _), (below, above) in zip(state, near):
        h1, h3 = (h + 1) % 4, (h + 3) % 4
        below.wait_recv()
        last.append(go.copy(at(h3, None, 0), at(h3, None, 0), me.device(high, 1)))
        above.wait_recv()
        last.append(go.copy(at(h1, None, 1), at(h1, None, 1), me.device(high, 3)))
    for made in last:
        made.wait_recv()
    out = []
    for m in range(3):
        out.append(pltpu.make_async_copy(scratch[m * per + 11], outs[m], local.at[3 + m]))
        out[-1].start()
    for made in out:
        made.wait()
    go.finish()


def reduced(terms):
    terms = [t.reshape(4, 2, t.shape[0] // 8, t.shape[1]) for t in terms]
    scratch = []
    for m, t in enumerate(terms):
        block = (4, *t.shape[2:])
        scratch += [pltpu.VMEM(block, BF16)] * 2
        for half, whole in plan(block, ROUTES[m][1]):
            scratch += [pltpu.VMEM(whole, F32), pltpu.VMEM((6, *half), BF16), pltpu.VMEM((6, *half), BF16)]
        scratch.append(pltpu.VMEM(t.shape[2:], BF16))
    hbm = pl.BlockSpec(memory_space=pltpu.HBM)
    return pl.pallas_call(
        reduce_kernel,
        out_shape=[jax.ShapeDtypeStruct(t.shape[2:], BF16) for t in terms],
        in_specs=[hbm] * 3,
        out_specs=[hbm] * 3,
        scratch_shapes=scratch
        + [
            pltpu.SemaphoreType.DMA((REDUCE_COPIES,)),
            pltpu.SemaphoreType.DMA((REDUCE_COPIES,)),
            pltpu.SemaphoreType.DMA((6,)),
        ],
        compiler_params=pltpu.CompilerParams(collective_id=1, has_side_effects=True, vmem_limit_bytes=60 * 2**20),
        name="reduce_gradients",
    )(*terms)


def solution(mesh):
    def fetched(weights, number):
        return {name: lax.all_gather(w[number], "s", axis=0, tiled=True) for name, w in zip(NAMES, weights, strict=True)}

    def summed(term):
        return lax.psum(lax.psum_scatter(term, "s", scatter_dimension=0, tiled=True), "r")

    def step(x, dy, *weights):
        h0 = x[0]
        w0 = dict(zip(NAMES, gathered(*(w[0] for w in weights))))
        w1 = fetched(weights, 1)
        h1 = layer(h0, w0)
        _, back = jax.vjp(lambda w, h: layer(h, w), w1, h1)
        by_w1, by_h = back(dy[0])
        mine1 = [summed(by_w1[name]) for name in NAMES]
        _, back = jax.vjp(lambda w, h: layer(h, w), w0, h0)
        by_w0, by_x = back(by_h)
        mine0 = reduced([by_w0[name] for name in NAMES])
        return (by_x[None], *(jnp.stack([a, b]) for a, b in zip(mine0, mine1)))

    states, cut = P(("rep", "r", "s"), None, None), P(None, "s", None)
    return jax.shard_map(
        step,
        mesh=mesh,
        in_specs=(states, states) + (cut,) * 3,
        out_specs=(states,) + (P("rep", "s", None),) * 3,
        check_vma=False,
    )
```

```python
import functools

import jax
import jax.numpy as jnp
from jax import lax
from jax.experimental import pallas as pl
from jax.experimental.pallas import tpu as pltpu
from jax.sharding import PartitionSpec as P

F32, BF16 = jnp.float32, jnp.bfloat16
MESH = pl.DeviceIdType.MESH


class Place:
    def __init__(self):
        rep, r, s = lax.axis_index("rep"), lax.axis_index("r"), lax.axis_index("s")
        self.c = s % 2
        at = {"x": s // 2, "y": r // 4, "z": r % 4}
        self.step = {a: [(at[a] + k) % 4 for k in range(4)] for a in "xyz"}

        def device(c, x, y, z):
            return (rep, y * 4 + z, x * 2 + c)

        self.other = device(1 - self.c, **at)
        self.who = {(a, k): device(self.c, **{**at, a: self.step[a][k]}) for a in "xyz" for k in (1, 2, 3)}

    def barrier(self):
        semaphore = pltpu.get_barrier_semaphore()
        for who in [self.other] + [self.who[a, k] for a in "xyz" for k in (1, 2, 3)]:
            pl.semaphore_signal(semaphore, inc=1, device_id=who, device_id_type=MESH)
        pl.semaphore_wait(semaphore, 10)


class Copy:
    def __init__(self, make):
        self.make = make

    def start(self):
        self.make().start()

    def wait(self):
        self.make().wait()

    def wait_recv(self):
        self.make().wait_recv()

    def wait_send(self):
        self.make().wait_send()


class Sender:
    def __init__(self, send, recv):
        self.send, self.recv, self.made = send, recv, []

    def copy(self, ends, who):
        k = len(self.made)

        def make():
            src, dst = ends()
            return pltpu.make_async_remote_copy(
                src_ref=src,
                dst_ref=dst,
                send_sem=self.send.at[k],
                recv_sem=self.recv.at[k],
                device_id=who,
                device_id_type=MESH,
            )

        self.made.append(Copy(make))
        return self.made[-1]

    def finish(self):
        for made in self.made:
            made.wait_send()


def run(phases, slots, position):
    for phase, (step, place) in zip(phases, slots, strict=True):
        if place == position:
            pl.when(pl.program_id(0) == step)(phase)


class Part:
    def __init__(self, own, out, axis, dim, base, size):
        self.own, self.out, self.axis, self.dim, self.base, self.size = own, out, axis, dim, base, size

    def cut(self, q, half):
        w = self.size // 4
        start = self.base + q * w
        if half is not None:
            w //= 2
            start = start + half * w
        return pl.ds(pl.multiple_of(start, w), w)

    def mine(self, q):
        d = self.cut(q, None)
        return self.own.at[:, d] if self.dim else self.own.at[d]

    def there(self, x, c, q, half=None):
        d = self.cut(q, half)
        return self.out.at[x, c, :, d] if self.dim else self.out.at[x, c, d]


GATHER_COPIES = 3 + 4 * 31


def gathering(me, go, owns, outs, local):
    c, other, who = me.c, me.other, me.who
    x, x1, x2, x3 = me.step["x"]
    (g, u, d), (og, ou, od) = owns, outs
    columns, rows = g.shape[1], d.shape[0]
    parts = [
        Part(g, og, "y", 1, 0, columns // 2),
        Part(g, og, "z", 1, columns // 2, columns // 2),
        Part(u, ou, "y", 1, 0, columns),
        Part(d, od, "z", 0, 0, rows),
    ]

    def own(i):
        return Copy(lambda: pltpu.make_async_copy(owns[i], outs[i].at[x, c], local.at[i]))

    def swap(i):
        return go.copy(lambda: (owns[i], outs[i].at[x, c]), other)

    def first(p, k):
        q = me.step[p.axis][0]
        return go.copy(lambda: (p.mine(q), p.there(x, c, q)), who["x", k])

    def on(p, at, q, half, to):
        return go.copy(lambda: (p.there(at, c, q, half), p.there(at, c, q, half)), to)

    here, swaps = [own(i) for i in range(3)], [swap(i) for i in range(3)]
    plans = []
    for p in parts:
        q, q1, q2, q3 = me.step[p.axis]
        up, down = who[p.axis, 1], who[p.axis, 3]
        plans.append(
            dict(
                first=[first(p, 1), first(p, 3)],
                second=[on(p, x3, q, 0, who["x", 1]), on(p, x1, q, 1, who["x", 3])],
                along=[[on(p, at, q, None, to) for to in (up, down)] for at in (x3, x1, x2)],
                across=[on(p, at, q, None, other) for at in (x3, x1, x2)],
                last=[[on(p, at, q3, 0, up), on(p, at, q1, 1, down)] for at in (x3, x1, x2)],
                across1=[[on(p, at, q3, None, other), on(p, at, q1, None, other)] for at in (x3, x1, x2)],
                across2=[[on(p, at, q2, half, other) for half in (0, 1)] for at in (x3, x1, x2)],
            )
        )

    def start():
        for i in here:
            i.start()
        me.barrier()
        for t in plans:
            for i in t["first"]:
                i.start()
        for i in swaps:
            i.start()

    def hand_on():
        for t in plans:
            for k in (0, 1):
                t["first"][k].wait_recv()
                t["second"][k].start()
                for i in t["along"][k]:
                    i.start()
                t["across"][k].start()

    def far():
        for t in plans:
            for i in t["second"]:
                i.wait_recv()
            for i in t["along"][2]:
                i.start()
            t["across"][2].start()

    def turn(k):
        def phase():
            for t in plans:
                for j in (0, 1):
                    t["along"][k][j].wait_recv()
                    t["last"][k][j].start()
                    t["across1"][k][j].start()

        return phase

    def ends(ks):
        def phase():
            for k in ks:
                for t in plans:
                    for j in (0, 1):
                        t["last"][k][j].wait_recv()
                        t["across2"][k][j].start()

        return phase

    def finish():
        for i in swaps:
            i.wait_recv()
        for t in plans:
            for i in t["across"] + sum(t["across1"] + t["across2"], []):
                i.wait_recv()
        for i in here:
            i.wait()
        go.finish()

    return [start, hand_on, far, turn(0), turn(1), turn(2), ends((0, 1, 2)), finish]


GATHER_SCRATCH = [
    pltpu.SemaphoreType.DMA((GATHER_COPIES,)),
    pltpu.SemaphoreType.DMA((GATHER_COPIES,)),
    pltpu.SemaphoreType.DMA((3,)),
]
HBM = pl.BlockSpec(memory_space=pltpu.HBM)


def rows_of(w, layer):
    return pl.BlockSpec((1, *w.shape[1:]), lambda *_: (layer, 0, 0), pipeline_mode=pl.Buffered(1))


def whole_shapes(weights):
    return [jax.ShapeDtypeStruct((4, 2, *w.shape[1:]), w.dtype) for w in weights]


def flat(ws):
    return [w.reshape(8 * w.shape[2], w.shape[3]) for w in ws]


def gather_kernel(g, u, d, og, ou, od, send, recv, local):
    for phase in gathering(Place(), Sender(send, recv), [w.at[0] for w in (g, u, d)], (og, ou, od), local):
        phase()


def gathered(weights, layer):
    return flat(
        pl.pallas_call(
            gather_kernel,
            grid=(1,),
            out_shape=whole_shapes(weights),
            in_specs=[rows_of(w, layer) for w in weights],
            out_specs=[HBM] * 3,
            scratch_shapes=GATHER_SCRATCH,
            compiler_params=pltpu.CompilerParams(collective_id=0, has_side_effects=True),
            name="gather_weights",
        )(*weights)
    )


def added(dst, *srcs):
    shape = dst.shape
    if len(shape) == 3:
        for i in range(shape[0]):
            added(dst.at[i], *(s.at[i] for s in srcs))
        return
    rows, columns = shape
    step = 16 if rows % 16 == 0 else rows
    wide = min(columns, 1024)

    @pl.loop(0, rows // step)
    def _(i):
        for j in range(0, columns, wide):
            at = (pl.ds(pl.multiple_of(i * step, step), step), pl.ds(j, min(wide, columns - j)))
            total = srcs[0][at].astype(F32)
            for s in srcs[1:]:
                total = total + s[at].astype(F32)
            dst[at] = total.astype(dst.dtype)


class Ring:
    def __init__(self, me, go, axis, terms, cut, out, got, hold):
        self.terms, self.cut, self.out, self.got = terms, cut, out, got
        self.at = me.step[axis]
        up, down = me.who[axis, 1], me.who[axis, 3]

        def slot(k, piece, half, to):
            def src():
                return cut(terms[1], self.at[piece], half) if hold is None else hold.at[k]

            return src, piece, half, go.copy(lambda: (src(), got.at[k]), to)

        self.slots = [
            slot(0, 2, 0, up),
            slot(1, 2, 1, down),
            slot(2, 1, 1, up),
            slot(3, 3, 0, down),
            slot(4, 1, 0, up),
            slot(5, 3, 1, down),
        ]

    def term(self, piece, half):
        return [self.cut(t, self.at[piece], half) for t in self.terms]

    def send(self, k, *more):
        src, piece, half, copy = self.slots[k]
        added(src(), *self.term(piece, half), *more)
        copy.start()

    def start(self):
        for k in range(4):
            self.send(k)

    def middle(self):
        for k in (0, 1):
            self.slots[k][3].wait_recv()
            self.send(4 + k, self.got.at[k])

    def end(self, cut_out):
        for k in (2, 3, 4, 5):
            self.slots[k][3].wait_recv()
        added(cut_out(self.out, 0), *self.term(0, 0), self.got.at[3], self.got.at[4])
        added(cut_out(self.out, 1), *self.term(0, 1), self.got.at[2], self.got.at[5])


def piece(dim, n):
    def cut(ref, q, half):
        w = ref.shape[dim] // 4
        at = [slice(None)] * len(ref.shape)
        if n == dim:
            at[dim] = pl.ds(pl.multiple_of(q * w + half * (w // 2), w // 2), w // 2)
        else:
            at[dim] = pl.ds(pl.multiple_of(q * w, w), w)
            h = ref.shape[n] // 2
            at[n] = pl.ds(half * h, h)
        if dim == 0 and len(ref.shape) == 3:
            at[0] = q
        return ref.at[tuple(at)]

    return cut


def halves(n):
    def cut(ref, half):
        h = ref.shape[n] // 2
        at = [slice(None)] * len(ref.shape)
        at[n] = pl.ds(half * h, h)
        return ref.at[tuple(at)]

    return cut


ROUTES = (
    (1, (("x", 0, 2), ("y", 1, 1), ("z", 1, 1))),
    (1, (("y", 2, 0), ("z", 2, 0), ("x", 0, 2))),
    (0, (("z", 1, 0), ("x", 0, 1), ("y", 0, 0))),
)


def plan(shape, steps):
    sizes = []
    for _, dim, n in steps:
        cut = list(shape)
        if dim == 0 and len(cut) == 3:
            cut = cut[1:]
            whole = list(cut)
            cut[n - 1] //= 2
        else:
            cut[dim] //= 4
            whole = list(cut)
            cut[n] //= 2
        sizes.append((tuple(cut), tuple(whole)))
        shape = tuple(whole)
    return sizes


REDUCE_COPIES = 3 * (1 + 18 + 3 + 4)


def reducing(me, go, terms, outs, scratch, local):
    c = me.c
    per = len(scratch) // 3
    bufs = [scratch[m * per : (m + 1) * per] for m in range(3)]

    def own(m):
        return Copy(lambda: pltpu.make_async_copy(terms[m].at[:, c], bufs[m][0], local.at[m]))

    def swap(m):
        return go.copy(lambda: (terms[m].at[:, 1 - c], bufs[m][1]), me.other)

    here, swaps = [own(m) for m in range(3)], [swap(m) for m in range(3)]
    rings = []
    for m in range(3):
        b, (_, steps) = bufs[m], ROUTES[m]
        made = []
        for k, (axis, dim, n) in enumerate(steps):
            t = (b[0], b[1]) if k == 0 else (made[-1].out,)
            at = 2 if k == 0 else 4 + 3 * (k - 1)
            made.append(Ring(me, go, axis, t, piece(dim, n), b[at], b[at + 1], None if k == 0 else b[at + 2]))
            made[-1].halves = halves(n - 1 if dim == 0 and len(t[0].shape) == 3 else n)
        rings.append(made)

    spread = []
    for m in range(3):
        dim, done = ROUTES[m][0], bufs[m][-1]
        size = done.shape[dim] // 16
        high, low = ("z", "y") if m == 2 else ("y", "z")

        def at(hi, lo=None, half=None, done=done, dim=dim, size=size):
            w = size if lo is not None else 4 * size
            start = hi * (4 * size) + (lo * size if lo is not None else 0)
            if half is not None:
                w //= 2
                start = start + half * w
            d = pl.ds(pl.multiple_of(start, w), w)
            return done.at[:, d] if dim else done.at[d]

        def copy(to, *where, at=at):
            return go.copy(lambda: (at(*where), at(*where)), to)

        h, h1, _, h3 = me.step[high]
        l = me.step[low][0]
        spread.append(
            dict(
                mine=lambda at=at, h=h, l=l: at(h, l),
                low=[copy(me.who[low, k], h, l) for k in (1, 2, 3)],
                near=[copy(me.who[high, 1], h), copy(me.who[high, 3], h)],
                far=[copy(me.who[high, 1], h3, None, 0), copy(me.who[high, 3], h1, None, 1)],
            )
        )
    back = [
        Copy(lambda m=m: pltpu.make_async_copy(bufs[m][-1], outs[m], local.at[3 + m])) for m in range(3)
    ]

    def start():
        for i in here:
            i.start()
        me.barrier()
        for i in swaps:
            i.start()

    def first(m):
        def phase():
            here[m].wait()
            swaps[m].wait_recv()
            rings[m][0].start()

        return phase

    def middle(k):
        def phase():
            for r in rings:
                r[k].middle()

        return phase

    def end(k):
        def phase():
            for r in rings:
                r[k].end(r[k].halves)
                if k < 2:
                    r[k + 1].start()

        return phase

    def low():
        end(2)()
        for m, t in enumerate(spread):
            added(t["mine"](), rings[m][2].out)
            for i in t["low"]:
                i.start()

    def near():
        for t in spread:
            for i in t["low"]:
                i.wait_recv()
            for i in t["near"]:
                i.start()

    def far():
        for k in (0, 1):
            for t in spread:
                t["near"][k].wait_recv()
                t["far"][k].start()

    def finish():
        for m, t in enumerate(spread):
            for i in t["far"]:
                i.wait_recv()
            back[m].start()
        for i in back:
            i.wait()
        go.finish()

    return [start, first(0), first(1), first(2), middle(0), end(0), middle(1), end(1), middle(2), low, near, far, finish]


def reduce_scratch(shapes):
    scratch = []
    for m, s in enumerate(shapes):
        block = (4, *s[2:])
        scratch += [pltpu.VMEM(block, BF16)] * 2
        for k, (half, whole) in enumerate(plan(block, ROUTES[m][1])):
            scratch += [pltpu.VMEM(whole, F32), pltpu.VMEM((6, *half), BF16)]
            if k:
                scratch.append(pltpu.VMEM((6, *half), BF16))
        scratch.append(pltpu.VMEM(s[2:], BF16))
    return scratch + [
        pltpu.SemaphoreType.DMA((REDUCE_COPIES,)),
        pltpu.SemaphoreType.DMA((REDUCE_COPIES,)),
        pltpu.SemaphoreType.DMA((6,)),
    ]


def blocks_of(terms):
    return [t.reshape(4, 2, t.shape[0] // 8, t.shape[1]) for t in terms]


def reduce_kernel(*refs):
    terms, outs, scratch = refs[:3], refs[3:6], refs[6:]
    send, recv, local = scratch[-3:]
    for phase in reducing(Place(), Sender(send, recv), terms, outs, scratch[:-3], local):
        phase()


def reduced(terms):
    terms = blocks_of(terms)
    return pl.pallas_call(
        reduce_kernel,
        out_shape=[jax.ShapeDtypeStruct(t.shape[2:], BF16) for t in terms],
        in_specs=[HBM] * 3,
        out_specs=[HBM] * 3,
        scratch_shapes=reduce_scratch([t.shape for t in terms]),
        compiler_params=pltpu.CompilerParams(collective_id=1, has_side_effects=True, vmem_limit_bytes=60 * 2**20),
        name="reduce_gradients",
    )(*terms)


def dot(a, b):
    return jnp.dot(a, b, preferred_element_type=F32)


def scale_of(wide):
    return lax.rsqrt(jnp.mean(wide * wide, -1, keepdims=True) + 1e-6)


def by_rows(tokens):
    def loop(body):
        @pl.loop(0, tokens // 256)
        def _(t):
            body(pl.ds(pl.multiple_of(t * 256, 256), 256))

    return loop


def dh_rows(h, dy, da, at):
    wide = h[at, :].astype(F32)
    scale = scale_of(wide)
    by_a = da[at, :].astype(BF16).astype(F32)
    inner = jnp.mean(by_a * wide, -1, keepdims=True)
    by_h = (by_a * scale - wide * (scale * scale * scale * inner)).astype(BF16)
    return dy[at, :] + by_h


FORWARD_SLOTS = ((0, 0), (2, 0), (3, 0), (3, 1), (4, 1), (5, 1), (6, 1), (7, 2))


def forward_kernel(tile, h, wg, wu, wd, ng, nu, nd, g_out, u_out, h_out, og, ou, od, a, acc, send, recv, local):
    i, n = pl.program_id(0), pl.num_programs(0)
    tokens = h.shape[0]
    phases = gathering(Place(), Sender(send, recv), [w.at[0] for w in (ng, nu, nd)], (og, ou, od), local)
    run(phases, FORWARD_SLOTS, 0)

    @pl.when(i == 0)
    def _():
        @by_rows(tokens)
        def _(at):
            wide = h[at, :].astype(F32)
            a[at, :] = (wide * scale_of(wide)).astype(BF16)
            acc[at, :] = jnp.zeros((256, h.shape[1]), F32)

    for t in range(tokens // tile):
        if t:
            run(phases, FORWARD_SLOTS, t)
        at = pl.ds(t * tile, tile)
        g = dot(a[at, :], wg[...])
        u = dot(a[at, :], wu[...])
        g_out[at, :] = g
        u_out[at, :] = u
        mid = (g * jax.nn.sigmoid(g) * u).astype(BF16)
        acc[at, :] += dot(mid, wd[...])

    @pl.when(i == n - 1)
    def _():
        @by_rows(tokens)
        def _(at):
            h_out[at, :] = h[at, :] + acc[at, :].astype(BF16)

    run(phases, FORWARD_SLOTS, 2)


def specs(tokens, d, chunk):
    whole = pl.BlockSpec((tokens, d), lambda i: (0, 0), pipeline_mode=pl.Buffered(1))
    across = pl.BlockSpec((d, chunk), lambda i: (0, i))
    down = pl.BlockSpec((chunk, d), lambda i: (i, 0))
    wide = pl.BlockSpec((tokens, chunk), lambda i: (0, i))
    return whole, across, down, wide


def first_of(tokens, d):
    return pl.BlockSpec((None, tokens, d), lambda i: (0, 0, 0), pipeline_mode=pl.Buffered(1))


def forward(x, w, weights, layer, chunk=512, tile=1024):
    _, tokens, d = x.shape
    ff = w[0].shape[1]
    whole, across, down, wide = specs(tokens, d, chunk)
    out = pl.pallas_call(
        functools.partial(forward_kernel, tile),
        grid=(ff // chunk,),
        out_shape=[jax.ShapeDtypeStruct((tokens, ff), F32)] * 2
        + [jax.ShapeDtypeStruct((tokens, d), BF16)]
        + whole_shapes(weights),
        in_specs=[first_of(tokens, d), across, across, down] + [rows_of(v, layer) for v in weights],
        out_specs=[wide, wide, whole] + [HBM] * 3,
        scratch_shapes=[pltpu.VMEM((tokens, d), BF16), pltpu.VMEM((tokens, d), F32)] + GATHER_SCRATCH,
        compiler_params=pltpu.CompilerParams(collective_id=1, has_side_effects=True, vmem_limit_bytes=60 * 2**20),
        name="forward_layer",
    )(x, *w, *weights)
    return out[0], out[1], out[2], flat(out[3:])


def backward_kernel(tile, h, dy, wg, wu, wd, dwg, dwu, dwd, dh, a, at_, dyt, da, mid, dg, du):
    i, n = pl.program_id(0), pl.num_programs(0)
    tokens = h.shape[0]

    @pl.when(i == 0)
    def _():
        @by_rows(tokens)
        def _(at):
            wide = h[at, :].astype(F32)
            rows = (wide * scale_of(wide)).astype(BF16)
            a[at, :] = rows
            at_[:, at] = rows.T
            dyt[:, at] = dy[at, :].T
            da[at, :] = jnp.zeros((256, h.shape[1]), F32)

    wdt, wgt, wut = wd[...].T, wg[...].T, wu[...].T
    for t in range(tokens // tile):
        at = pl.ds(t * tile, tile)
        g = dot(a[at, :], wg[...])
        u = dot(a[at, :], wu[...])
        dm = dot(dy[at, :], wdt).astype(BF16).astype(F32)
        sg = jax.nn.sigmoid(g)
        s = g * sg
        mid[at, :] = (s * u).astype(BF16)
        dub = (dm * s).astype(BF16)
        dgb = (dm * u * (sg + s * (1.0 - sg))).astype(BF16)
        du[at, :] = dub
        dg[at, :] = dgb
        da[at, :] += dot(dgb, wgt) + dot(dub, wut)
    dwg[...] = dot(at_[...], dg[...]).astype(BF16)
    dwu[...] = dot(at_[...], du[...]).astype(BF16)
    dwd[...] = dot(dyt[...], mid[...]).T.astype(BF16)

    @pl.when(i == n - 1)
    def _():
        @by_rows(tokens)
        def _(at):
            dh[at, :] = dh_rows(h, dy, da, at)


def backward(h, dy, w, chunk=512, tile=1024):
    tokens, d = h.shape
    ff = w[0].shape[1]
    whole, across, down, wide = specs(tokens, d, chunk)
    return pl.pallas_call(
        functools.partial(backward_kernel, tile),
        grid=(ff // chunk,),
        out_shape=[jax.ShapeDtypeStruct((d, ff), BF16)] * 2
        + [jax.ShapeDtypeStruct((ff, d), BF16), jax.ShapeDtypeStruct((tokens, d), BF16)],
        in_specs=[whole, first_of(tokens, d), across, across, down],
        out_specs=[across, across, down, whole],
        scratch_shapes=[
            pltpu.VMEM((tokens, d), BF16),
            pltpu.VMEM((d, tokens), BF16),
            pltpu.VMEM((d, tokens), BF16),
            pltpu.VMEM((tokens, d), F32),
        ]
        + [pltpu.VMEM((tokens, chunk), BF16)] * 3,
        compiler_params=pltpu.CompilerParams(vmem_limit_bytes=62 * 2**20),
        name="backward_layer",
    )(h, dy, *w)


WEIGHTS_SLOTS = (
    ((0, 0), (2, 0), (3, 0), (4, 0), (5, 0), (7, 0), (8, 0), (9, 0), (10, 0), (11, 0), (12, 0), (13, 0), (15, 2))
)


def weights_kernel(tile, h, dy, wd, g, u, t0, t1, t2, dwg, dwu, dwd, dg, du, o0, o1, o2, at_, dyt, mid, *scratch):
    i = pl.program_id(0)
    tokens = h.shape[0]
    send, recv, local = scratch[-3:]
    phases = reducing(Place(), Sender(send, recv), (t0, t1, t2), (o0, o1, o2), scratch[:-3], local)
    run(phases, WEIGHTS_SLOTS, 0)

    @pl.when(i == 0)
    def _():
        @by_rows(tokens)
        def _(at):
            wide = h[at, :].astype(F32)
            at_[:, at] = (wide * scale_of(wide)).astype(BF16).T
            dyt[:, at] = dy[at, :].T

    wdt = wd[...].T
    for t in range(tokens // tile):
        at = pl.ds(t * tile, tile)
        gg, uu = g[at, :], u[at, :]
        dm = dot(dy[at, :], wdt).astype(BF16).astype(F32)
        sg = jax.nn.sigmoid(gg)
        s = gg * sg
        mid[at, :] = (s * uu).astype(BF16)
        du[at, :] = (dm * s).astype(BF16)
        dg[at, :] = (dm * uu * (sg + s * (1.0 - sg))).astype(BF16)
    dwg[...] = dot(at_[...], dg[...]).astype(BF16)
    dwu[...] = dot(at_[...], du[...]).astype(BF16)
    dwd[...] = dot(dyt[...], mid[...]).T.astype(BF16)
    run(phases, WEIGHTS_SLOTS, 2)


def weights_back(x, dy, wd, g, u, terms, chunk=256, tile=512):
    _, tokens, d = x.shape
    ff = wd.shape[0]
    whole, across, down, wide = specs(tokens, d, chunk)
    terms = blocks_of(terms)
    out = pl.pallas_call(
        functools.partial(weights_kernel, tile),
        grid=(ff // chunk,),
        out_shape=[jax.ShapeDtypeStruct((d, ff), BF16)] * 2
        + [jax.ShapeDtypeStruct((ff, d), BF16)]
        + [jax.ShapeDtypeStruct((tokens, ff), BF16)] * 2
        + [jax.ShapeDtypeStruct(t.shape[2:], BF16) for t in terms],
        in_specs=[first_of(tokens, d), whole, down, wide, wide] + [HBM] * 3,
        out_specs=[across, across, down, wide, wide] + [HBM] * 3,
        scratch_shapes=[pltpu.VMEM((d, tokens), BF16)] * 2
        + [pltpu.VMEM((tokens, chunk), BF16)]
        + reduce_scratch([t.shape for t in terms]),
        compiler_params=pltpu.CompilerParams(collective_id=2, has_side_effects=True, vmem_limit_bytes=67043328),
        name="weights_back",
    )(x, dy, wd, g, u, *terms)
    return out[:3], out[3], out[4], out[5:]


INPUT_SLOTS = (
    ((0, 0), (1, 0), (2, 0), (3, 0), (4, 0), (6, 0), (7, 0), (7, 2), (7, 2), (7, 2), (7, 2), (7, 2), (7, 2))
)


def input_kernel(tile, h, dy, wg, wu, dg, du, t0, t1, t2, dx, o0, o1, o2, da, *scratch):
    i, n = pl.program_id(0), pl.num_programs(0)
    tokens = h.shape[0]
    send, recv, local = scratch[-3:]
    phases = reducing(Place(), Sender(send, recv), (t0, t1, t2), (o0, o1, o2), scratch[:-3], local)
    run(phases, INPUT_SLOTS, 0)

    @pl.when(i == 0)
    def _():
        @by_rows(tokens)
        def _(at):
            da[at, :] = jnp.zeros((256, h.shape[1]), F32)

    wgt, wut = wg[...].T, wu[...].T
    for t in range(tokens // tile):
        at = pl.ds(t * tile, tile)
        da[at, :] += dot(dg[at, :], wgt) + dot(du[at, :], wut)

    @pl.when(i == n - 1)
    def _():
        @by_rows(tokens)
        def _(at):
            dx[at, :] = dh_rows(h, dy, da, at)

    run(phases, INPUT_SLOTS, 2)


def input_back(x, dy, wg, wu, dg, du, terms, chunk=512, tile=1024):
    _, tokens, d = x.shape
    ff = wg.shape[1]
    whole, across, down, wide = specs(tokens, d, chunk)
    terms = blocks_of(terms)
    out = pl.pallas_call(
        functools.partial(input_kernel, tile),
        grid=(ff // chunk,),
        out_shape=[jax.ShapeDtypeStruct(x.shape, BF16)] + [jax.ShapeDtypeStruct(t.shape[2:], BF16) for t in terms],
        in_specs=[first_of(tokens, d), whole, across, across, wide, wide] + [HBM] * 3,
        out_specs=[first_of(tokens, d)] + [HBM] * 3,
        scratch_shapes=[pltpu.VMEM((tokens, d), F32)] + reduce_scratch([t.shape for t in terms]),
        compiler_params=pltpu.CompilerParams(collective_id=3, has_side_effects=True, vmem_limit_bytes=67043328),
        name="input_back",
    )(x, dy, wg, wu, dg, du, *terms)
    return out[0], out[1:]


def solution(mesh):
    def step(x, dy, *weights):
        w0 = gathered(weights, 0)
        g0, u0, h1, w1 = forward(x, w0, weights, 1)
        *terms1, by_h = backward(h1, dy, w1)
        terms0, dg, du, mine1 = weights_back(x, by_h, w0[2], g0, u0, terms1)
        by_x, mine0 = input_back(x, by_h, w0[0], w0[1], dg, du, terms0)
        return (by_x, *(jnp.stack([a, b]) for a, b in zip(mine0, mine1)))

    states, cut = P(("rep", "r", "s"), None, None), P(None, "s", None)
    return jax.shard_map(
        step,
        mesh=mesh,
        in_specs=(states, states) + (cut,) * 3,
        out_specs=(states,) + (P("rep", "s", None),) * 3,
        check_vma=False,
    )
```

```python
import functools

import jax
import jax.numpy as jnp
from jax import lax
from jax.experimental import pallas as pl
from jax.experimental.pallas import tpu as pltpu
from jax.sharding import PartitionSpec as P

F32, BF16 = jnp.float32, jnp.bfloat16
MESH = pl.DeviceIdType.MESH


class Place:
    def __init__(self):
        rep, r, s = lax.axis_index("rep"), lax.axis_index("r"), lax.axis_index("s")
        self.c = s % 2
        at = {"x": s // 2, "y": r // 4, "z": r % 4}
        self.step = {a: [(at[a] + k) % 4 for k in range(4)] for a in "xyz"}

        def device(c, x, y, z):
            return (rep, y * 4 + z, x * 2 + c)

        self.other = device(1 - self.c, **at)
        self.who = {(a, k): device(self.c, **{**at, a: self.step[a][k]}) for a in "xyz" for k in range(1, 4)}

    def barrier(self):
        semaphore = pltpu.get_barrier_semaphore()
        for who in [self.other] + [self.who[a, k] for a in "xyz" for k in range(1, 4)]:
            pl.semaphore_signal(semaphore, inc=1, device_id=who, device_id_type=MESH)
        pl.semaphore_wait(semaphore, 10)

    def greet(self):
        semaphore = pltpu.get_barrier_semaphore()
        pl.semaphore_signal(semaphore, inc=1, device_id=self.other, device_id_type=MESH)
        pl.semaphore_wait(semaphore, 1)


class Copy:
    def __init__(self, make):
        self.make = make

    def start(self):
        self.make().start()

    def wait(self):
        self.make().wait()

    def wait_recv(self):
        self.make().wait_recv()

    def wait_send(self):
        self.make().wait_send()


class Sender:
    def __init__(self, send, recv):
        self.send, self.recv, self.made = send, recv, []

    def copy(self, ends, who):
        k = len(self.made)

        def make():
            src, dst = ends()
            return pltpu.make_async_remote_copy(
                src_ref=src,
                dst_ref=dst,
                send_sem=self.send.at[k],
                recv_sem=self.recv.at[k],
                device_id=who,
                device_id_type=MESH,
            )

        self.made.append(Copy(make))
        return self.made[-1]

    def finish(self):
        for made in self.made:
            made.wait_send()


class Swap:
    def __init__(self, me, held, outs, send, recv, chunk):
        self.me, self.held, self.outs, self.send, self.recv, self.chunk = me, held, outs, send, recv, chunk
        self.rows = outs[2].shape[1]

    def theirs(self, i):
        return (i * self.chunk // self.rows) % 2 != self.me.c

    def copy(self, k, i):
        first = i * self.chunk
        if k < 2:
            dst = self.outs[k].at[:, :, pl.ds(pl.multiple_of(first, self.chunk), self.chunk)]
        else:
            dst = self.outs[2].at[first // self.rows // 2, pl.ds(pl.multiple_of(first % self.rows, self.chunk), self.chunk)]
        return pltpu.make_async_remote_copy(
            src_ref=self.held[k],
            dst_ref=dst,
            send_sem=self.send.at[k],
            recv_sem=self.recv.at[k, i],
            device_id=self.me.other,
            device_id_type=MESH,
        )

    def sent(self, i):
        for k in (0, 1):
            self.copy(k, i).wait_send()
        pl.when(self.theirs(i))(lambda: self.copy(2, i).wait_send())

    def step(self, i, n, *made):
        pl.when(i > 0)(lambda: self.sent(i - 1))
        block = made[0].shape[0] // 8
        for k in (0, 1):
            for x in range(4):
                at = pl.multiple_of((2 * x + 1 - self.me.c) * block, 16)
                self.held[k][x] = made[k][pl.ds(at, block), :]
            self.copy(k, i).start()

        @pl.when(self.theirs(i))
        def _():
            self.held[2][...] = made[2][...]
            self.copy(2, i).start()

        @pl.when(i == n - 1)
        def _():
            self.sent(i)
            for j in range(n):
                for k in (0, 1):
                    self.copy(k, j).wait_recv()
                pl.when(jnp.logical_not(self.theirs(j)))(lambda: self.copy(2, j).wait_recv())


def swap_scratch(d, ff, chunk):
    held = [pltpu.VMEM((4, d // 8, chunk), BF16)] * 2 + [pltpu.VMEM((chunk, d), BF16)]
    return held + [pltpu.SemaphoreType.DMA((3,)), pltpu.SemaphoreType.DMA((3, ff // chunk))]


def swap_shapes(d, ff):
    return [jax.ShapeDtypeStruct((4, d // 8, ff), BF16)] * 2 + [jax.ShapeDtypeStruct((4, ff // 8, d), BF16)]


def run(phases, slots, position, steps):
    for phase, slot in zip(phases, slots, strict=True):
        step, place = (steps - 1, 2) if slot == 2 * steps else divmod(slot, 2)
        if place == position:
            pl.when(pl.program_id(0) == step)(phase)


class Part:
    def __init__(self, own, out, axis, dim, base, size):
        self.own, self.out, self.axis, self.dim, self.base, self.size = own, out, axis, dim, base, size

    def cut(self, q, half):
        w = self.size // 4
        start = self.base + q * w
        if half is not None:
            w //= 2
            start = start + half * w
        return pl.ds(pl.multiple_of(start, w), w)

    def mine(self, q):
        d = self.cut(q, None)
        return self.own.at[:, d] if self.dim else self.own.at[d]

    def there(self, x, c, q, half=None):
        d = self.cut(q, half)
        return self.out.at[x, c, :, d] if self.dim else self.out.at[x, c, d]


GATHER_COPIES = 3 + 4 * 28


def gathering(me, go, owns, outs, local):
    c, other, who = me.c, me.other, me.who
    x, x1, x2, x3 = me.step["x"]
    (g, u, d), (og, ou, od) = owns, outs
    columns, rows = g.shape[1], d.shape[0]
    parts = [
        Part(g, og, "y", 1, 0, columns // 2),
        Part(g, og, "z", 1, columns // 2, columns // 2),
        Part(u, ou, "y", 1, 0, columns),
        Part(d, od, "z", 0, 0, rows),
    ]

    def own(i):
        return Copy(lambda: pltpu.make_async_copy(owns[i], outs[i].at[x, c], local.at[i]))

    def swap(i):
        return go.copy(lambda: (owns[i], outs[i].at[x, c]), other)

    def first(p, k):
        q = me.step[p.axis][0]
        return go.copy(lambda: (p.mine(q), p.there(x, c, q)), who["x", k])

    def on(p, at, q, half, to):
        return go.copy(lambda: (p.there(at, c, q, half), p.there(at, c, q, half)), to)

    here, swaps = [own(i) for i in range(3)], [swap(i) for i in range(3)]
    plans = []
    for p in parts:
        q, q1, q2, q3 = me.step[p.axis]
        up, down = who[p.axis, 1], who[p.axis, 3]
        plans.append(
            dict(
                first=[first(p, 1), first(p, 3)],
                second=[on(p, x3, q, 0, who["x", 1]), on(p, x1, q, 1, who["x", 3])],
                along=[[on(p, at, q, None, to) for to in (up, down)] for at in (x3, x1, x2)],
                across=[on(p, at, q, None, other) for at in (x3, x1, x2)],
                passed=[[on(p, at, k, None, other) for k in (q3, q1)] for at in (x3, x1, x2)],
                whole=[on(p, at, q2, None, other) for at in (x3, x1, x2)],
                last=[[on(p, at, q3, 0, up), on(p, at, q1, 1, down)] for at in (x3, x1, x2)],
            )
        )

    def start():
        for i in here:
            i.start()
        me.barrier()
        for t in plans:
            for i in t["first"]:
                i.start()
        for i in swaps:
            i.start()

    def hand_on():
        for t in plans:
            for k in (0, 1):
                t["first"][k].wait_recv()
                t["second"][k].start()
                for i in [*t["along"][k], t["across"][k]]:
                    i.start()

    def far():
        for t in plans:
            for i in t["second"]:
                i.wait_recv()
            for i in [*t["along"][2], t["across"][2]]:
                i.start()

    def turn(k):
        def phase():
            for t in plans:
                for j in (0, 1):
                    t["along"][k][j].wait_recv()
                    t["last"][k][j].start()
                    t["passed"][k][j].start()

        return phase

    def ends():
        for k in range(3):
            for t in plans:
                for i in t["last"][k]:
                    i.wait_recv()
                t["whole"][k].start()

    def finish():
        for i in swaps:
            i.wait_recv()
        for t in plans:
            for i in t["across"] + sum(t["passed"], t["whole"]):
                i.wait_recv()
        for i in here:
            i.wait()
        go.finish()

    return [start, hand_on, far, turn(0), turn(1), turn(2), ends, finish]


GATHER_SCRATCH = [
    pltpu.SemaphoreType.DMA((GATHER_COPIES,)),
    pltpu.SemaphoreType.DMA((GATHER_COPIES,)),
    pltpu.SemaphoreType.DMA((3,)),
]
HBM = pl.BlockSpec(memory_space=pltpu.HBM)


def rows_of(w, layer):
    return pl.BlockSpec((1, *w.shape[1:]), lambda *_: (layer, 0, 0), pipeline_mode=pl.Buffered(1))


def whole_shapes(weights):
    return [jax.ShapeDtypeStruct((4, 2, *w.shape[1:]), w.dtype) for w in weights]


def flat(ws):
    return [w.reshape(8 * w.shape[2], w.shape[3]) for w in ws]


def gather_kernel(g, u, d, og, ou, od, send, recv, local):
    for phase in gathering(Place(), Sender(send, recv), [w.at[0] for w in (g, u, d)], (og, ou, od), local):
        phase()


def gathered(weights, layer):
    return flat(
        pl.pallas_call(
            gather_kernel,
            grid=(1,),
            out_shape=whole_shapes(weights),
            in_specs=[rows_of(w, layer) for w in weights],
            out_specs=[HBM] * 3,
            scratch_shapes=GATHER_SCRATCH,
            compiler_params=pltpu.CompilerParams(collective_id=0, has_side_effects=True),
            name="gather_weights",
        )(*weights)
    )


def added(dst, *srcs):
    shape = dst.shape
    if len(shape) == 3:
        for i in range(shape[0]):
            added(dst.at[i], *(s.at[i] for s in srcs))
        return
    rows, columns = shape
    wide = 512 if columns > 1024 else columns
    tall = rows
    while tall * wide > 49152 and tall % 32 == 0:
        tall //= 2

    def block(i, j):
        at = (pl.ds(pl.multiple_of(i, 16), tall), pl.ds(pl.multiple_of(j, 128), wide))
        total = srcs[0][at].astype(F32)
        for s in srcs[1:]:
            total = total + s[at].astype(F32)
        dst[at] = total.astype(dst.dtype)

    if wide < columns:
        pl.loop(0, columns // wide)(lambda j: block(0, j * wide))
    else:
        for i in range(rows // tall):
            block(i * tall, 0)


class Ring:
    def __init__(self, me, go, axis, terms, cut, out, got, hold):
        self.terms, self.cut, self.out, self.got = terms, cut, out, got
        self.at = me.step[axis]
        up, down = me.who[axis, 1], me.who[axis, 3]

        def slot(k, piece, half, to):
            def src():
                return cut(terms[1], self.at[piece], half) if hold is None else hold.at[k]

            return src, piece, half, go.copy(lambda: (src(), got.at[k]), to)

        order = ((2, 0), (2, 1), (1, 1), (3, 0), (1, 0), (3, 1))
        self.slots = [slot(k, *which, down if k % 2 else up) for k, which in enumerate(order)]

    def term(self, piece, half):
        return [self.cut(t, self.at[piece], half) for t in self.terms]

    def send(self, k, *more):
        src, piece, half, copy = self.slots[k]
        added(src(), *self.term(piece, half), *more)
        copy.start()

    def start(self):
        for k in range(4):
            self.send(k)

    def middle(self):
        for k in (0, 1):
            self.slots[k][3].wait_recv()
            self.send(4 + k, self.got.at[k])

    def end(self, cut_out):
        for k in range(2, 6):
            self.slots[k][3].wait_recv()
        added(cut_out(self.out, 0), *self.term(0, 0), self.got.at[3], self.got.at[4])
        added(cut_out(self.out, 1), *self.term(0, 1), self.got.at[2], self.got.at[5])


class Direct:
    def __init__(self, me, go, axis, terms, cut, out, got, hold):
        self.term, self.cut, self.out, self.got, self.hold, self.at = terms[0], cut, out, got, hold, me.step[axis]
        self.sent = [self.copy(go, k, me.who[axis, k + 1]) for k in range(3)]

    def copy(self, go, k, to):
        return go.copy(lambda: (self.hold.at[k], self.got.at[k]), to)

    def start(self):
        for k, copy in enumerate(self.sent):
            added(self.hold.at[k], self.cut(self.term, self.at[k + 1], None))
            copy.start()

    def end(self, _):
        for copy in self.sent:
            copy.wait_recv()
        added(self.out, self.cut(self.term, self.at[0], None), *(self.got.at[k] for k in range(3)))


def piece(dim, n):
    def cut(ref, q, half):
        w = ref.shape[dim] // 4
        at = [slice(None)] * len(ref.shape)
        if n == dim and half is not None:
            at[dim] = pl.ds(pl.multiple_of(q * w + half * (w // 2), w // 2), w // 2)
        else:
            at[dim] = pl.ds(pl.multiple_of(q * w, w), w)
            if half is not None:
                h = ref.shape[n] // 2
                at[n] = pl.ds(half * h, h)
        if dim == 0 and len(ref.shape) == 3:
            at[0] = q
        return ref.at[tuple(at)]

    return cut


def halves(n):
    def cut(ref, half):
        h = ref.shape[n] // 2
        at = [slice(None)] * len(ref.shape)
        at[n] = pl.ds(half * h, h)
        return ref.at[tuple(at)]

    return cut


ROUTES = (
    (1, (("x", 0, 2), ("y", 1, 1), ("z", 1, 1))),
    (1, (("y", 2, 0), ("z", 2, 0), ("x", 0, 2))),
    (0, (("z", 1, 0), ("x", 0, 1), ("y", 0, 0))),
)


def plan(shape, steps):
    sizes = []
    for _, dim, n in steps:
        cut = list(shape)
        if dim == 0 and len(cut) == 3:
            cut = cut[1:]
            whole = list(cut)
            cut[n - 1] //= 2
        else:
            cut[dim] //= 4
            whole = list(cut)
            cut[n] //= 2
        sizes.append((tuple(cut), tuple(whole)))
        shape = tuple(whole)
    return sizes


REDUCE_COPIES = 3 * (12 + 3 + 3 + 4)


def reducing(me, go, terms, arrived, outs, scratch, local):
    c = me.c
    per = len(scratch) // 3
    bufs = [scratch[m * per : (m + 1) * per] for m in range(3)]

    def own(m):
        return Copy(lambda: pltpu.make_async_copy(terms[m].at[:, c], bufs[m][0], local.at[m]))

    def swap(m):
        return Copy(lambda: pltpu.make_async_copy(arrived[m], bufs[m][1], local.at[6 + m]))

    here, swaps = [own(m) for m in range(3)], [swap(m) for m in range(3)]
    rings = []
    for m in range(3):
        b, (_, steps) = bufs[m], ROUTES[m]
        made = []
        for k, (axis, dim, n) in enumerate(steps):
            t = (b[0], b[1]) if k == 0 else (made[-1].out,)
            at = 2 if k == 0 else 4 + 3 * (k - 1)
            kind = Ring if k < 2 else Direct
            made.append(kind(me, go, axis, t, piece(dim, n), b[at], b[at + 1], b[at + 2] if k else None))
            made[-1].halves = halves(n - 1 if dim == 0 and len(t[0].shape) == 3 else n)
        rings.append(made)

    spread = []
    for m in range(3):
        dim, done = ROUTES[m][0], bufs[m][-1]
        size = done.shape[dim] // 16
        high, low = ("z", "y") if m == 2 else ("y", "z")

        def at(hi, lo=None, half=None, done=done, dim=dim, size=size):
            w = size if lo is not None else 4 * size
            start = hi * (4 * size) + (lo * size if lo is not None else 0)
            if half is not None:
                w //= 2
                start = start + half * w
            d = pl.ds(pl.multiple_of(start, w), w)
            return done.at[:, d] if dim else done.at[d]

        def copy(to, *where, at=at):
            return go.copy(lambda: (at(*where), at(*where)), to)

        h, h1, _, h3 = me.step[high]
        l = me.step[low][0]
        spread.append(
            dict(
                mine=lambda at=at, h=h, l=l: at(h, l),
                low=[copy(me.who[low, k], h, l) for k in range(1, 4)],
                near=[copy(me.who[high, 1], h), copy(me.who[high, 3], h)],
                far=[copy(me.who[high, 1], h3, None, 0), copy(me.who[high, 3], h1, None, 1)],
            )
        )
    back = [
        Copy(lambda m=m: pltpu.make_async_copy(bufs[m][-1], outs[m], local.at[3 + m])) for m in range(3)
    ]

    def start():
        for m in range(3):
            here[m].start()
            swaps[m].start()
        me.barrier()

    def first(m):
        def phase():
            here[m].wait()
            swaps[m].wait()
            rings[m][0].start()

        return phase

    def middle(k):
        def phase():
            for r in rings:
                r[k].middle()

        return phase

    def end(k):
        def phase():
            for r in rings:
                r[k].end(r[k].halves)
                if k < 2:
                    r[k + 1].start()

        return phase

    def low():
        end(2)()
        for m, t in enumerate(spread):
            added(t["mine"](), rings[m][2].out)
            for i in t["low"]:
                i.start()

    def near():
        for t in spread:
            for i in t["low"]:
                i.wait_recv()
            for i in t["near"]:
                i.start()

    def far():
        for k in (0, 1):
            for t in spread:
                t["near"][k].wait_recv()
                t["far"][k].start()

    def finish():
        for m, t in enumerate(spread):
            for i in t["far"]:
                i.wait_recv()
            back[m].start()
        for i in back:
            i.wait()
        go.finish()

    return [start, first(0), first(1), first(2), middle(0), end(0), middle(1), end(1), low, near, far, finish]


def reduce_scratch(shapes):
    scratch = []
    for m, s in enumerate(shapes):
        block = (4, *s[2:])
        scratch += [pltpu.VMEM(block, BF16)] * 2
        for k, (half, whole) in enumerate(plan(block, ROUTES[m][1])):
            many = (6, *half) if k < 2 else (3, *whole)
            scratch += [pltpu.VMEM(whole, F32)] + [pltpu.VMEM(many, BF16)] * (2 if k else 1)
        scratch.append(pltpu.VMEM(s[2:], BF16))
    return scratch + [
        pltpu.SemaphoreType.DMA((REDUCE_COPIES,)),
        pltpu.SemaphoreType.DMA((REDUCE_COPIES,)),
        pltpu.SemaphoreType.DMA((9,)),
    ]


def blocks_of(terms):
    return [t.reshape(4, 2, t.shape[0] // 8, t.shape[1]) for t in terms]


def dot(a, b):
    return jnp.dot(a, b, preferred_element_type=F32)


def scale_of(wide):
    return lax.rsqrt(jnp.mean(wide * wide, -1, keepdims=True) + 1e-6)


def by_rows(tokens):
    def loop(body):
        @pl.loop(0, tokens // 256)
        def _(t):
            body(pl.ds(pl.multiple_of(t * 256, 256), 256))

    return loop


def dh_rows(h, dy, da, at):
    wide = h[at, :].astype(F32)
    scale = scale_of(wide)
    by_a = da[at, :].astype(BF16).astype(F32)
    inner = jnp.mean(by_a * wide, -1, keepdims=True)
    by_h = (by_a * scale - wide * (scale * scale * scale * inner)).astype(BF16)
    return dy[at, :] + by_h


FORWARD_SLOTS = (0, 4, 6, 7, 9, 11, 13, 16)


def forward_kernel(tile, steps, h, wg, wu, wd, ng, nu, nd, g_out, u_out, h_out, og, ou, od, a, acc, send, recv, local):
    i, n = pl.program_id(0), pl.num_programs(0)
    tokens = h.shape[0]
    phases = gathering(Place(), Sender(send, recv), [w.at[0] for w in (ng, nu, nd)], (og, ou, od), local)
    run(phases, FORWARD_SLOTS, 0, steps)

    @pl.when(i == 0)
    def _():
        @by_rows(tokens)
        def _(at):
            wide = h[at, :].astype(F32)
            a[at, :] = (wide * scale_of(wide)).astype(BF16)
            acc[at, :] = jnp.zeros((256, h.shape[1]), F32)

    for t in range(tokens // tile):
        if t:
            run(phases, FORWARD_SLOTS, t, steps)
        at = pl.ds(t * tile, tile)
        g = dot(a[at, :], wg[...])
        u = dot(a[at, :], wu[...])
        g_out[at, :] = g
        u_out[at, :] = u
        mid = (g * jax.nn.sigmoid(g) * u).astype(BF16)
        acc[at, :] += dot(mid, wd[...])

    @pl.when(i == n - 1)
    def _():
        @by_rows(tokens)
        def _(at):
            h_out[at, :] = h[at, :] + acc[at, :].astype(BF16)

    run(phases, FORWARD_SLOTS, 2, steps)


def specs(tokens, d, chunk):
    whole = pl.BlockSpec((tokens, d), lambda i: (0, 0), pipeline_mode=pl.Buffered(1))
    across = pl.BlockSpec((d, chunk), lambda i: (0, i))
    down = pl.BlockSpec((chunk, d), lambda i: (i, 0))
    wide = pl.BlockSpec((tokens, chunk), lambda i: (0, i))
    return whole, across, down, wide


def first_of(tokens, d):
    return pl.BlockSpec((None, tokens, d), lambda i: (0, 0, 0), pipeline_mode=pl.Buffered(1))


def forward(x, w, weights, layer, chunk=512, tile=1024):
    _, tokens, d = x.shape
    ff = w[0].shape[1]
    whole, across, down, wide = specs(tokens, d, chunk)
    out = pl.pallas_call(
        functools.partial(forward_kernel, tile, ff // chunk),
        grid=(ff // chunk,),
        out_shape=[jax.ShapeDtypeStruct((tokens, ff), F32)] * 2
        + [jax.ShapeDtypeStruct((tokens, d), BF16)]
        + whole_shapes(weights),
        in_specs=[first_of(tokens, d), across, across, down] + [rows_of(v, layer) for v in weights],
        out_specs=[wide, wide, whole] + [HBM] * 3,
        scratch_shapes=[pltpu.VMEM((tokens, d), BF16), pltpu.VMEM((tokens, d), F32)] + GATHER_SCRATCH,
        compiler_params=pltpu.CompilerParams(collective_id=1, has_side_effects=True, vmem_limit_bytes=60 * 2**20),
        name="forward_layer",
    )(x, *w, *weights)
    return out[0], out[1], out[2], flat(out[3:])


def backward_kernel(
    tile, steps, h, dy, wg, wu, wd, dwg, dwu, dwd, dh, r0, r1, r2, a, at_, dyt, da, mid, dg, du, h0, h1, h2, send, recv
):
    i, n = pl.program_id(0), pl.num_programs(0)
    tokens, chunk = h.shape[0], wg.shape[1]
    me = Place()
    swap = Swap(me, (h0, h1, h2), (r0, r1, r2), send, recv, chunk)
    pl.when(i == 0)(me.greet)

    @pl.when(i == 0)
    def _():
        @by_rows(tokens)
        def _(at):
            wide = h[at, :].astype(F32)
            rows = (wide * scale_of(wide)).astype(BF16)
            a[at, :] = rows
            at_[:, at] = rows.T
            dyt[:, at] = dy[at, :].T
            da[at, :] = jnp.zeros((256, h.shape[1]), F32)

    wdt, wgt, wut = wd[...].T, wg[...].T, wu[...].T
    for t in range(tokens // tile):
        at = pl.ds(t * tile, tile)
        g = dot(a[at, :], wg[...])
        u = dot(a[at, :], wu[...])
        dm = dot(dy[at, :], wdt).astype(BF16).astype(F32)
        sg = jax.nn.sigmoid(g)
        s = g * sg
        mid[at, :] = (s * u).astype(BF16)
        dub = (dm * s).astype(BF16)
        dgb = (dm * u * (sg + s * (1.0 - sg))).astype(BF16)
        du[at, :] = dub
        dg[at, :] = dgb
        da[at, :] += dot(dgb, wgt) + dot(dub, wut)
    dwg[...] = dot(at_[...], dg[...]).astype(BF16)
    dwu[...] = dot(at_[...], du[...]).astype(BF16)
    dwd[...] = dot(dyt[...], mid[...]).T.astype(BF16)

    @pl.when(i == n - 1)
    def _():
        @by_rows(tokens)
        def _(at):
            dh[at, :] = dh_rows(h, dy, da, at)

    swap.step(i, steps, dwg, dwu, dwd)


def backward(h, dy, w, chunk=512, tile=1024):
    tokens, d = h.shape
    ff = w[0].shape[1]
    whole, across, down, wide = specs(tokens, d, chunk)
    out = pl.pallas_call(
        functools.partial(backward_kernel, tile, ff // chunk),
        grid=(ff // chunk,),
        out_shape=[jax.ShapeDtypeStruct((d, ff), BF16)] * 2
        + [jax.ShapeDtypeStruct((ff, d), BF16), jax.ShapeDtypeStruct((tokens, d), BF16)]
        + swap_shapes(d, ff),
        in_specs=[whole, first_of(tokens, d), across, across, down],
        out_specs=[across, across, down, whole] + [HBM] * 3,
        scratch_shapes=[
            pltpu.VMEM((tokens, d), BF16),
            pltpu.VMEM((d, tokens), BF16),
            pltpu.VMEM((d, tokens), BF16),
            pltpu.VMEM((tokens, d), F32),
        ]
        + [pltpu.VMEM((tokens, chunk), BF16)] * 3
        + swap_scratch(d, ff, chunk),
        compiler_params=pltpu.CompilerParams(collective_id=4, has_side_effects=True, vmem_limit_bytes=67043328),
        name="backward_layer",
    )(h, dy, *w)
    return out[:3], out[3], out[4:]


WEIGHTS_SLOTS = (0, *(2,) * 3, 8, 14, 16, 20, 24, 26, 30, 32)


def weights_kernel(tile, steps, h, dy, wd, g, u, *refs):
    refs = iter(refs)
    terms, arrived, (dwg, dwu, dwd), (dg, du), outs, swapped, (at_, dyt, mid), held, (to, come) = (
        [next(refs) for _ in name] for name in ("tgu", "rgu", "gud", "gu", "ogu", "sgu", "adm", "hgu", "tc")
    )
    scratch = list(refs)
    i = pl.program_id(0)
    tokens, chunk = h.shape[0], wd.shape[0]
    send, recv, local = scratch[-3:]
    me = Place()
    swap = Swap(me, held, swapped, to, come, chunk)
    phases = reducing(me, Sender(send, recv), terms, arrived, outs, scratch[:-3], local)
    run(phases, WEIGHTS_SLOTS, 0, steps)

    @pl.when(i == 0)
    def _():
        @by_rows(tokens)
        def _(at):
            wide = h[at, :].astype(F32)
            at_[:, at] = (wide * scale_of(wide)).astype(BF16).T
            dyt[:, at] = dy[at, :].T

    wdt = wd[...].T
    for t in range(tokens // tile):
        at = pl.ds(t * tile, tile)
        gg, uu = g[at, :], u[at, :]
        dm = dot(dy[at, :], wdt).astype(BF16).astype(F32)
        sg = jax.nn.sigmoid(gg)
        s = gg * sg
        mid[at, :] = (s * uu).astype(BF16)
        du[at, :] = (dm * s).astype(BF16)
        dg[at, :] = (dm * uu * (sg + s * (1.0 - sg))).astype(BF16)
    dwg[...] = dot(at_[...], dg[...]).astype(BF16)
    dwu[...] = dot(at_[...], du[...]).astype(BF16)
    dwd[...] = dot(dyt[...], mid[...]).T.astype(BF16)
    swap.step(i, steps, dwg, dwu, dwd)
    run(phases, WEIGHTS_SLOTS, 2, steps)


def weights_back(x, dy, wd, g, u, terms, arrived, chunk=256, tile=512):
    _, tokens, d = x.shape
    ff = wd.shape[0]
    whole, across, down, wide = specs(tokens, d, chunk)
    terms = blocks_of(terms)
    out = pl.pallas_call(
        functools.partial(weights_kernel, tile, ff // chunk),
        grid=(ff // chunk,),
        out_shape=[jax.ShapeDtypeStruct((d, ff), BF16)] * 2
        + [jax.ShapeDtypeStruct((ff, d), BF16)]
        + [jax.ShapeDtypeStruct((tokens, ff), BF16)] * 2
        + [jax.ShapeDtypeStruct(t.shape[2:], BF16) for t in terms]
        + swap_shapes(d, ff),
        in_specs=[first_of(tokens, d), whole, down, wide, wide] + [HBM] * 6,
        out_specs=[across, across, down, wide, wide] + [HBM] * 6,
        scratch_shapes=[pltpu.VMEM((d, tokens), BF16)] * 2
        + [pltpu.VMEM((tokens, chunk), BF16)]
        + swap_scratch(d, ff, chunk)
        + reduce_scratch([t.shape for t in terms]),
        compiler_params=pltpu.CompilerParams(collective_id=2, has_side_effects=True, vmem_limit_bytes=67043328),
        name="weights_back",
    )(x, dy, wd, g, u, *terms, *arrived)
    return out[:3], out[3], out[4], out[5:8], out[8:]


INPUT_SLOTS = (0, *(2,) * 3, 6, 10, 12, 14, *(16,) * 4)


def input_kernel(tile, steps, h, dy, wg, wu, dg, du, t0, t1, t2, r0, r1, r2, dx, o0, o1, o2, da, *scratch):
    i, n = pl.program_id(0), pl.num_programs(0)
    tokens = h.shape[0]
    send, recv, local = scratch[-3:]
    phases = reducing(Place(), Sender(send, recv), (t0, t1, t2), (r0, r1, r2), (o0, o1, o2), scratch[:-3], local)
    run(phases, INPUT_SLOTS, 0, steps)

    @pl.when(i == 0)
    def _():
        @by_rows(tokens)
        def _(at):
            da[at, :] = jnp.zeros((256, h.shape[1]), F32)

    wgt, wut = wg[...].T, wu[...].T
    for t in range(tokens // tile):
        if t:
            run(phases, INPUT_SLOTS, t, steps)
        at = pl.ds(t * tile, tile)
        da[at, :] += dot(dg[at, :], wgt) + dot(du[at, :], wut)

    @pl.when(i == n - 1)
    def _():
        @by_rows(tokens)
        def _(at):
            dx[at, :] = dh_rows(h, dy, da, at)

    run(phases, INPUT_SLOTS, 2, steps)


def input_back(x, dy, wg, wu, dg, du, terms, arrived, chunk=512, tile=1024):
    _, tokens, d = x.shape
    ff = wg.shape[1]
    whole, across, down, wide = specs(tokens, d, chunk)
    terms = blocks_of(terms)
    out = pl.pallas_call(
        functools.partial(input_kernel, tile, ff // chunk),
        grid=(ff // chunk,),
        out_shape=[jax.ShapeDtypeStruct(x.shape, BF16)] + [jax.ShapeDtypeStruct(t.shape[2:], BF16) for t in terms],
        in_specs=[first_of(tokens, d), whole, across, across, wide, wide] + [HBM] * 6,
        out_specs=[first_of(tokens, d)] + [HBM] * 3,
        scratch_shapes=[pltpu.VMEM((tokens, d), F32)] + reduce_scratch([t.shape for t in terms]),
        compiler_params=pltpu.CompilerParams(collective_id=3, has_side_effects=True, vmem_limit_bytes=67043328),
        name="input_back",
    )(x, dy, wg, wu, dg, du, *terms, *arrived)
    return out[0], out[1:]


def solution(mesh):
    def step(x, dy, *weights):
        w0 = gathered(weights, 0)
        g0, u0, h1, w1 = forward(x, w0, weights, 1)
        terms1, by_h, arrived1 = backward(h1, dy, w1)
        terms0, dg, du, mine1, arrived0 = weights_back(x, by_h, w0[2], g0, u0, terms1, arrived1)
        by_x, mine0 = input_back(x, by_h, w0[0], w0[1], dg, du, terms0, arrived0)
        return (by_x, *(jnp.stack([a, b]) for a, b in zip(mine0, mine1)))

    states, cut = P(("rep", "r", "s"), None, None), P(None, "s", None)
    return jax.shard_map(
        step,
        mesh=mesh,
        in_specs=(states, states) + (cut,) * 3,
        out_specs=(states,) + (P("rep", "s", None),) * 3,
        check_vma=False,
    )
```

```python
import functools

import jax
import jax.numpy as jnp
from jax import lax
from jax.experimental import pallas as pl
from jax.experimental.pallas import tpu as pltpu
from jax.sharding import PartitionSpec as P

F32, BF16 = jnp.float32, jnp.bfloat16
MESH = pl.DeviceIdType.MESH


class Place:
    def __init__(self):
        rep, r, s = lax.axis_index("rep"), lax.axis_index("r"), lax.axis_index("s")
        self.c = s % 2
        at = {"x": s // 2, "y": r // 4, "z": r % 4}
        self.step = {a: [(at[a] + k) % 4 for k in range(4)] for a in "xyz"}

        def device(c, x, y, z):
            return (rep, y * 4 + z, x * 2 + c)

        self.other = device(1 - self.c, **at)
        self.who = {(a, k): device(self.c, **{**at, a: self.step[a][k]}) for a in "xyz" for k in range(1, 4)}

    def barrier(self):
        semaphore = pltpu.get_barrier_semaphore()
        for who in [self.other] + [self.who[a, k] for a in "xyz" for k in range(1, 4)]:
            pl.semaphore_signal(semaphore, inc=1, device_id=who, device_id_type=MESH)
        pl.semaphore_wait(semaphore, 10)

    def greet(self):
        semaphore = pltpu.get_barrier_semaphore()
        pl.semaphore_signal(semaphore, inc=1, device_id=self.other, device_id_type=MESH)
        pl.semaphore_wait(semaphore, 1)


class Copy:
    def __init__(self, make):
        self.make = make

    def start(self):
        self.make().start()

    def wait(self):
        self.make().wait()

    def wait_recv(self):
        self.make().wait_recv()

    def wait_send(self):
        self.make().wait_send()


class Sender:
    def __init__(self, send, recv):
        self.send, self.recv, self.made = send, recv, []

    def copy(self, ends, who):
        k = len(self.made)

        def make():
            src, dst = ends()
            return pltpu.make_async_remote_copy(
                src_ref=src,
                dst_ref=dst,
                send_sem=self.send.at[k],
                recv_sem=self.recv.at[k],
                device_id=who,
                device_id_type=MESH,
            )

        self.made.append(Copy(make))
        return self.made[-1]

    def finish(self):
        for made in self.made:
            made.wait_send()


class Swap:
    def __init__(self, me, held, outs, send, recv, chunk):
        self.me, self.held, self.outs, self.send, self.recv, self.chunk = me, held, outs, send, recv, chunk
        self.rows = outs[2].shape[1]

    def theirs(self, i):
        return (i * self.chunk // self.rows) % 2 != self.me.c

    def copy(self, k, i):
        first = i * self.chunk
        if k < 2:
            dst = self.outs[k].at[:, :, pl.ds(pl.multiple_of(first, self.chunk), self.chunk)]
        else:
            dst = self.outs[2].at[first // self.rows // 2, pl.ds(pl.multiple_of(first % self.rows, self.chunk), self.chunk)]
        return pltpu.make_async_remote_copy(
            src_ref=self.held[k],
            dst_ref=dst,
            send_sem=self.send.at[k],
            recv_sem=self.recv.at[k, i],
            device_id=self.me.other,
            device_id_type=MESH,
        )

    def sent(self, i):
        for k in (0, 1):
            self.copy(k, i).wait_send()
        pl.when(self.theirs(i))(lambda: self.copy(2, i).wait_send())

    def step(self, i, n, *made):
        pl.when(i > 0)(lambda: self.sent(i - 1))
        block = made[0].shape[0] // 8
        for k in (0, 1):
            for x in range(4):
                at = pl.multiple_of((2 * x + 1 - self.me.c) * block, 16)
                self.held[k][x] = made[k][pl.ds(at, block), :]
            self.copy(k, i).start()

        @pl.when(self.theirs(i))
        def _():
            self.held[2][...] = made[2][...]
            self.copy(2, i).start()

        @pl.when(i == n - 1)
        def _():
            self.sent(i)
            for j in range(n):
                for k in (0, 1):
                    self.copy(k, j).wait_recv()
                pl.when(jnp.logical_not(self.theirs(j)))(lambda: self.copy(2, j).wait_recv())


def swap_scratch(d, ff, chunk):
    held = [pltpu.VMEM((4, d // 8, chunk), BF16)] * 2 + [pltpu.VMEM((chunk, d), BF16)]
    return held + [pltpu.SemaphoreType.DMA((3,)), pltpu.SemaphoreType.DMA((3, ff // chunk))]


def swap_shapes(d, ff):
    return [jax.ShapeDtypeStruct((4, d // 8, ff), BF16)] * 2 + [jax.ShapeDtypeStruct((4, ff // 8, d), BF16)]


def run(phases, slots, position, steps):
    for phase, slot in zip(phases, slots, strict=True):
        step, place = (steps - 1, 2) if slot == 2 * steps else divmod(slot, 2)
        if place == position:
            pl.when(pl.program_id(0) == step)(phase)


class Part:
    def __init__(self, own, out, axis, dim, base, size):
        self.own, self.out, self.axis, self.dim, self.base, self.size = own, out, axis, dim, base, size

    def cut(self, q, half):
        w = self.size // 4
        start = self.base + q * w
        if half is not None:
            w //= 2
            start = start + half * w
        return pl.ds(pl.multiple_of(start, w), w)

    def mine(self, q):
        d = self.cut(q, None)
        return self.own.at[:, d] if self.dim else self.own.at[d]

    def there(self, x, c, q, half=None):
        d = self.cut(q, half)
        return self.out.at[x, c, :, d] if self.dim else self.out.at[x, c, d]


GATHER_COPIES = 3 + 4 * 28


def gathering(me, go, owns, outs, local):
    c, other, who = me.c, me.other, me.who
    x, x1, x2, x3 = me.step["x"]
    (g, u, d), (og, ou, od) = owns, outs
    columns, rows = g.shape[1], d.shape[0]
    parts = [
        Part(g, og, "y", 1, 0, columns // 2),
        Part(g, og, "z", 1, columns // 2, columns // 2),
        Part(u, ou, "y", 1, 0, columns),
        Part(d, od, "z", 0, 0, rows),
    ]

    def own(i):
        return Copy(lambda: pltpu.make_async_copy(owns[i], outs[i].at[x, c], local.at[i]))

    def swap(i):
        return go.copy(lambda: (owns[i], outs[i].at[x, c]), other)

    def first(p, k):
        q = me.step[p.axis][0]
        return go.copy(lambda: (p.mine(q), p.there(x, c, q)), who["x", k])

    def on(p, at, q, half, to):
        return go.copy(lambda: (p.there(at, c, q, half), p.there(at, c, q, half)), to)

    here, swaps = [own(i) for i in range(3)], [swap(i) for i in range(3)]
    plans = []
    for p in parts:
        q, q1, q2, q3 = me.step[p.axis]
        up, down = who[p.axis, 1], who[p.axis, 3]
        plans.append(
            dict(
                first=[first(p, 1), first(p, 3)],
                second=[on(p, x3, q, 0, who["x", 1]), on(p, x1, q, 1, who["x", 3])],
                along=[[on(p, at, q, None, to) for to in (up, down)] for at in (x3, x1, x2)],
                across=[on(p, at, q, None, other) for at in (x3, x1, x2)],
                passed=[[on(p, at, k, None, other) for k in (q3, q1)] for at in (x3, x1, x2)],
                whole=[on(p, at, q2, None, other) for at in (x3, x1, x2)],
                last=[[on(p, at, q3, 0, up), on(p, at, q1, 1, down)] for at in (x3, x1, x2)],
            )
        )

    def start():
        for i in here:
            i.start()
        me.barrier()
        for t in plans:
            for i in t["first"]:
                i.start()
        for i in swaps:
            i.start()

    def hand_on():
        for t in plans:
            for k in (0, 1):
                t["first"][k].wait_recv()
                t["second"][k].start()
                for i in [*t["along"][k], t["across"][k]]:
                    i.start()

    def far():
        for t in plans:
            for i in t["second"]:
                i.wait_recv()
            for i in [*t["along"][2], t["across"][2]]:
                i.start()

    def turn(k):
        def phase():
            for t in plans:
                for j in (0, 1):
                    t["along"][k][j].wait_recv()
                    t["last"][k][j].start()
                    t["passed"][k][j].start()

        return phase

    def ends():
        for k in range(3):
            for t in plans:
                for i in t["last"][k]:
                    i.wait_recv()
                t["whole"][k].start()

    def finish():
        for i in swaps:
            i.wait_recv()
        for t in plans:
            for i in t["across"] + sum(t["passed"], t["whole"]):
                i.wait_recv()
        for i in here:
            i.wait()
        go.finish()

    return [start, hand_on, far, turn(0), turn(1), turn(2), ends, finish]


GATHER_SCRATCH = [
    pltpu.SemaphoreType.DMA((GATHER_COPIES,)),
    pltpu.SemaphoreType.DMA((GATHER_COPIES,)),
    pltpu.SemaphoreType.DMA((3,)),
]
HBM = pl.BlockSpec(memory_space=pltpu.HBM)


def rows_of(w, layer):
    return pl.BlockSpec((1, *w.shape[1:]), lambda *_: (layer, 0, 0), pipeline_mode=pl.Buffered(1))


def whole_shapes(weights):
    return [jax.ShapeDtypeStruct((4, 2, *w.shape[1:]), w.dtype) for w in weights]


def flat(ws):
    return [w.reshape(8 * w.shape[2], w.shape[3]) for w in ws]


def gather_kernel(g, u, d, og, ou, od, send, recv, local):
    for phase in gathering(Place(), Sender(send, recv), [w.at[0] for w in (g, u, d)], (og, ou, od), local):
        phase()


def gathered(weights, layer):
    return flat(
        pl.pallas_call(
            gather_kernel,
            grid=(1,),
            out_shape=whole_shapes(weights),
            in_specs=[rows_of(w, layer) for w in weights],
            out_specs=[HBM] * 3,
            scratch_shapes=GATHER_SCRATCH,
            compiler_params=pltpu.CompilerParams(collective_id=0, has_side_effects=True),
            name="gather_weights",
        )(*weights)
    )


def added(dst, *srcs):
    shape = dst.shape
    if len(shape) == 3:
        for i in range(shape[0]):
            added(dst.at[i], *(s.at[i] for s in srcs))
        return
    rows, columns = shape
    wide = 512 if columns > 1024 else columns
    tall = rows
    while tall * wide > 49152 and tall % 32 == 0:
        tall //= 2

    def block(i, j):
        at = (pl.ds(pl.multiple_of(i, 16), tall), pl.ds(pl.multiple_of(j, 128), wide))
        total = srcs[0][at].astype(F32)
        for s in srcs[1:]:
            total = total + s[at].astype(F32)
        dst[at] = total.astype(dst.dtype)

    if wide < columns:
        pl.loop(0, columns // wide)(lambda j: block(0, j * wide))
    else:
        for i in range(rows // tall):
            block(i * tall, 0)


class Ring:
    def __init__(self, me, go, axis, terms, cut, out, got, hold):
        self.terms, self.cut, self.out, self.got = terms, cut, out, got
        self.at = me.step[axis]
        up, down = me.who[axis, 1], me.who[axis, 3]

        def slot(k, piece, half, to):
            def src():
                return cut(terms[1], self.at[piece], half) if hold is None else hold.at[k]

            return src, piece, half, go.copy(lambda: (src(), got.at[k]), to)

        order = ((2, 0), (2, 1), (1, 1), (3, 0), (1, 0), (3, 1))
        self.slots = [slot(k, *which, down if k % 2 else up) for k, which in enumerate(order)]

    def term(self, piece, half):
        return [self.cut(t, self.at[piece], half) for t in self.terms]

    def send(self, k, *more):
        src, piece, half, copy = self.slots[k]
        added(src(), *self.term(piece, half), *more)
        copy.start()

    def start(self):
        for k in range(4):
            self.send(k)

    def middle(self):
        for k in (0, 1):
            self.slots[k][3].wait_recv()
            self.send(4 + k, self.got.at[k])

    def end(self, cut_out):
        for k in range(2, 6):
            self.slots[k][3].wait_recv()
        added(cut_out(self.out, 0), *self.term(0, 0), self.got.at[3], self.got.at[4])
        added(cut_out(self.out, 1), *self.term(0, 1), self.got.at[2], self.got.at[5])


class Direct:
    def __init__(self, me, go, axis, terms, cut, out, got, hold):
        self.term, self.cut, self.out, self.got, self.hold, self.at = terms[0], cut, out, got, hold, me.step[axis]
        self.sent = [self.copy(go, k, me.who[axis, k + 1]) for k in range(3)]

    def copy(self, go, k, to):
        return go.copy(lambda: (self.hold.at[k], self.got.at[k]), to)

    def start(self):
        for k, copy in enumerate(self.sent):
            added(self.hold.at[k], self.cut(self.term, self.at[k + 1], None))
            copy.start()

    def end(self, _):
        for copy in self.sent:
            copy.wait_recv()
        added(self.out, self.cut(self.term, self.at[0], None), *(self.got.at[k] for k in range(3)))


def piece(dim, n):
    def cut(ref, q, half):
        w = ref.shape[dim] // 4
        at = [slice(None)] * len(ref.shape)
        if n == dim and half is not None:
            at[dim] = pl.ds(pl.multiple_of(q * w + half * (w // 2), w // 2), w // 2)
        else:
            at[dim] = pl.ds(pl.multiple_of(q * w, w), w)
            if half is not None:
                h = ref.shape[n] // 2
                at[n] = pl.ds(half * h, h)
        if dim == 0 and len(ref.shape) == 3:
            at[0] = q
        return ref.at[tuple(at)]

    return cut


def halves(n):
    def cut(ref, half):
        h = ref.shape[n] // 2
        at = [slice(None)] * len(ref.shape)
        at[n] = pl.ds(half * h, h)
        return ref.at[tuple(at)]

    return cut


ROUTES = (
    (1, (("x", 0, 2), ("y", 1, 1), ("z", 1, 1))),
    (1, (("y", 2, 0), ("z", 2, 0), ("x", 0, 2))),
    (0, (("z", 1, 0), ("x", 0, 1), ("y", 0, 0))),
)


def plan(shape, steps):
    sizes = []
    for _, dim, n in steps:
        cut = list(shape)
        if dim == 0 and len(cut) == 3:
            cut = cut[1:]
            whole = list(cut)
            cut[n - 1] //= 2
        else:
            cut[dim] //= 4
            whole = list(cut)
            cut[n] //= 2
        sizes.append((tuple(cut), tuple(whole)))
        shape = tuple(whole)
    return sizes


REDUCE_COPIES = 3 * (12 + 3 + 3 + 4)


def reducing(me, go, terms, arrived, outs, scratch, local):
    c = me.c
    per = len(scratch) // 3
    bufs = [scratch[m * per : (m + 1) * per] for m in range(3)]

    def own(m):
        return Copy(lambda: pltpu.make_async_copy(terms[m].at[:, c], bufs[m][0], local.at[m]))

    def swap(m):
        return Copy(lambda: pltpu.make_async_copy(arrived[m], bufs[m][1], local.at[6 + m]))

    here, swaps = [own(m) for m in range(3)], [swap(m) for m in range(3)]
    rings = []
    for m in range(3):
        b, (_, steps) = bufs[m], ROUTES[m]
        made = []
        for k, (axis, dim, n) in enumerate(steps):
            t = (b[0], b[1]) if k == 0 else (made[-1].out,)
            at = 2 if k == 0 else 4 + 3 * (k - 1)
            kind = Ring if k < 2 else Direct
            made.append(kind(me, go, axis, t, piece(dim, n), b[at], b[at + 1], b[at + 2] if k else None))
            made[-1].halves = halves(n - 1 if dim == 0 and len(t[0].shape) == 3 else n)
        rings.append(made)

    spread = []
    for m in range(3):
        dim, done = ROUTES[m][0], bufs[m][-1]
        size = done.shape[dim] // 16
        high, low = ("z", "y") if m == 2 else ("y", "z")

        def at(hi, lo=None, half=None, done=done, dim=dim, size=size):
            w = size if lo is not None else 4 * size
            start = hi * (4 * size) + (lo * size if lo is not None else 0)
            if half is not None:
                w //= 2
                start = start + half * w
            d = pl.ds(pl.multiple_of(start, w), w)
            return done.at[:, d] if dim else done.at[d]

        def copy(to, *where, at=at):
            return go.copy(lambda: (at(*where), at(*where)), to)

        h, h1, _, h3 = me.step[high]
        l = me.step[low][0]
        spread.append(
            dict(
                mine=lambda at=at, h=h, l=l: at(h, l),
                low=[copy(me.who[low, k], h, l) for k in range(1, 4)],
                near=[copy(me.who[high, 1], h), copy(me.who[high, 3], h)],
                far=[copy(me.who[high, 1], h3, None, 0), copy(me.who[high, 3], h1, None, 1)],
            )
        )
    back = [
        Copy(lambda m=m: pltpu.make_async_copy(bufs[m][-1], outs[m], local.at[3 + m])) for m in range(3)
    ]

    def start():
        for m in range(3):
            here[m].start()
            swaps[m].start()
        me.barrier()

    def first(m):
        def phase():
            here[m].wait()
            swaps[m].wait()
            rings[m][0].start()

        return phase

    def middle(k):
        def phase():
            for r in rings:
                r[k].middle()

        return phase

    def end(k):
        def phase():
            for r in rings:
                r[k].end(r[k].halves)
                if k < 2:
                    r[k + 1].start()

        return phase

    def low():
        end(2)()
        for m, t in enumerate(spread):
            added(t["mine"](), rings[m][2].out)
            for i in t["low"]:
                i.start()

    def near():
        for t in spread:
            for i in t["low"]:
                i.wait_recv()
            for i in t["near"]:
                i.start()

    def far():
        for k in (0, 1):
            for t in spread:
                t["near"][k].wait_recv()
                t["far"][k].start()

    def finish():
        for m, t in enumerate(spread):
            for i in t["far"]:
                i.wait_recv()
            back[m].start()
        for i in back:
            i.wait()
        go.finish()

    return [start, first(0), first(1), first(2), middle(0), end(0), middle(1), end(1), low, near, far, finish]


def reduce_scratch(shapes):
    scratch = []
    for m, s in enumerate(shapes):
        block = (4, *s[2:])
        scratch += [pltpu.VMEM(block, BF16)] * 2
        for k, (half, whole) in enumerate(plan(block, ROUTES[m][1])):
            many = (6, *half) if k < 2 else (3, *whole)
            scratch += [pltpu.VMEM(whole, F32)] + [pltpu.VMEM(many, BF16)] * (2 if k else 1)
        scratch.append(pltpu.VMEM(s[2:], BF16))
    return scratch + [
        pltpu.SemaphoreType.DMA((REDUCE_COPIES,)),
        pltpu.SemaphoreType.DMA((REDUCE_COPIES,)),
        pltpu.SemaphoreType.DMA((9,)),
    ]


def blocks_of(terms):
    return [t.reshape(4, 2, t.shape[0] // 8, t.shape[1]) for t in terms]


def dot(a, b):
    return jnp.dot(a, b, preferred_element_type=F32)


def scale_of(wide):
    return lax.rsqrt(jnp.mean(wide * wide, -1, keepdims=True) + 1e-6)


def by_rows(tokens):
    def loop(body):
        @pl.loop(0, tokens // 256)
        def _(t):
            body(pl.ds(pl.multiple_of(t * 256, 256), 256))

    return loop


def dh_rows(h, dy, da, at):
    wide = h[at, :].astype(F32)
    scale = scale_of(wide)
    by_a = da[at, :].astype(BF16).astype(F32)
    inner = jnp.mean(by_a * wide, -1, keepdims=True)
    by_h = (by_a * scale - wide * (scale * scale * scale * inner)).astype(BF16)
    return dy[at, :] + by_h


FORWARD_SLOTS = (0, 4, 6, 7, 9, 11, 13, 16)


def forward_kernel(tile, steps, h, wg, wu, wd, ng, nu, nd, g_out, u_out, h_out, og, ou, od, a, acc, send, recv, local):
    i, n = pl.program_id(0), pl.num_programs(0)
    tokens = h.shape[0]
    phases = gathering(Place(), Sender(send, recv), [w.at[0] for w in (ng, nu, nd)], (og, ou, od), local)
    run(phases, FORWARD_SLOTS, 0, steps)

    @pl.when(i == 0)
    def _():
        @by_rows(tokens)
        def _(at):
            wide = h[at, :].astype(F32)
            a[at, :] = (wide * scale_of(wide)).astype(BF16)
            acc[at, :] = jnp.zeros((256, h.shape[1]), F32)

    for t in range(tokens // tile):
        if t:
            run(phases, FORWARD_SLOTS, t, steps)
        at = pl.ds(t * tile, tile)
        g = dot(a[at, :], wg[...])
        u = dot(a[at, :], wu[...])
        g_out[at, :] = g
        u_out[at, :] = u
        mid = (g * jax.nn.sigmoid(g) * u).astype(BF16)
        acc[at, :] += dot(mid, wd[...])

    @pl.when(i == n - 1)
    def _():
        @by_rows(tokens)
        def _(at):
            h_out[at, :] = h[at, :] + acc[at, :].astype(BF16)

    run(phases, FORWARD_SLOTS, 2, steps)


def specs(tokens, d, chunk):
    whole = pl.BlockSpec((tokens, d), lambda i: (0, 0), pipeline_mode=pl.Buffered(1))
    across = pl.BlockSpec((d, chunk), lambda i: (0, i))
    down = pl.BlockSpec((chunk, d), lambda i: (i, 0))
    wide = pl.BlockSpec((tokens, chunk), lambda i: (0, i))
    return whole, across, down, wide


def first_of(tokens, d):
    return pl.BlockSpec((None, tokens, d), lambda i: (0, 0, 0), pipeline_mode=pl.Buffered(1))


def forward(x, w, weights, layer, chunk=512, tile=1024):
    _, tokens, d = x.shape
    ff = w[0].shape[1]
    whole, across, down, wide = specs(tokens, d, chunk)
    out = pl.pallas_call(
        functools.partial(forward_kernel, tile, ff // chunk),
        grid=(ff // chunk,),
        out_shape=[jax.ShapeDtypeStruct((tokens, ff), F32)] * 2
        + [jax.ShapeDtypeStruct((tokens, d), BF16)]
        + whole_shapes(weights),
        in_specs=[first_of(tokens, d), across, across, down] + [rows_of(v, layer) for v in weights],
        out_specs=[wide, wide, whole] + [HBM] * 3,
        scratch_shapes=[pltpu.VMEM((tokens, d), BF16), pltpu.VMEM((tokens, d), F32)] + GATHER_SCRATCH,
        compiler_params=pltpu.CompilerParams(collective_id=1, has_side_effects=True, vmem_limit_bytes=60 * 2**20),
        name="forward_layer",
    )(x, *w, *weights)
    return out[0], out[1], out[2], flat(out[3:])


def backward_kernel(
    tile, steps, h, dy, wg, wu, wd, dwg, dwu, dwd, dh, r0, r1, r2, a, at_, dyt, da, mid, dg, du, h0, h1, h2, send, recv
):
    i, n = pl.program_id(0), pl.num_programs(0)
    tokens, chunk = h.shape[0], wg.shape[1]
    me = Place()
    swap = Swap(me, (h0, h1, h2), (r0, r1, r2), send, recv, chunk)
    pl.when(i == 0)(me.greet)

    @pl.when(i == 0)
    def _():
        @by_rows(tokens)
        def _(at):
            wide = h[at, :].astype(F32)
            rows = (wide * scale_of(wide)).astype(BF16)
            a[at, :] = rows
            at_[:, at] = rows.T
            dyt[:, at] = dy[at, :].T
            da[at, :] = jnp.zeros((256, h.shape[1]), F32)

    wdt, wgut = wd[...].T, jnp.concatenate([wg[...], wu[...]], 1).T
    for t in range(tokens // tile):
        at = pl.ds(t * tile, tile)
        g = dot(a[at, :], wg[...])
        u = dot(a[at, :], wu[...])
        dm = dot(dy[at, :], wdt).astype(BF16).astype(F32)
        sg = jax.nn.sigmoid(g)
        s = g * sg
        mid[at, :] = (s * u).astype(BF16)
        dub = (dm * s).astype(BF16)
        dgb = (dm * u * (sg + s * (1.0 - sg))).astype(BF16)
        du[at, :] = dub
        dg[at, :] = dgb
        da[at, :] += dot(jnp.concatenate([dgb, dub], 1), wgut)
    dwg[...] = dot(at_[...], dg[...]).astype(BF16)
    dwu[...] = dot(at_[...], du[...]).astype(BF16)
    dwd[...] = dot(dyt[...], mid[...]).T.astype(BF16)

    @pl.when(i == n - 1)
    def _():
        @by_rows(tokens)
        def _(at):
            dh[at, :] = dh_rows(h, dy, da, at)

    swap.step(i, steps, dwg, dwu, dwd)


def backward(h, dy, w, chunk=512, tile=1024):
    tokens, d = h.shape
    ff = w[0].shape[1]
    whole, across, down, wide = specs(tokens, d, chunk)
    out = pl.pallas_call(
        functools.partial(backward_kernel, tile, ff // chunk),
        grid=(ff // chunk,),
        out_shape=[jax.ShapeDtypeStruct((d, ff), BF16)] * 2
        + [jax.ShapeDtypeStruct((ff, d), BF16), jax.ShapeDtypeStruct((tokens, d), BF16)]
        + swap_shapes(d, ff),
        in_specs=[whole, first_of(tokens, d), across, across, down],
        out_specs=[across, across, down, whole] + [HBM] * 3,
        scratch_shapes=[
            pltpu.VMEM((tokens, d), BF16),
            pltpu.VMEM((d, tokens), BF16),
            pltpu.VMEM((d, tokens), BF16),
            pltpu.VMEM((tokens, d), F32),
        ]
        + [pltpu.VMEM((tokens, chunk), BF16)] * 3
        + swap_scratch(d, ff, chunk),
        compiler_params=pltpu.CompilerParams(collective_id=4, has_side_effects=True, vmem_limit_bytes=67043328),
        name="backward_layer",
    )(h, dy, *w)
    return out[:3], out[3], out[4:]


WEIGHTS_SLOTS = (0, *(2,) * 3, 8, 14, 16, 20, 24, 26, 30, 32)


def weights_kernel(tile, steps, h, dy, wd, g, u, *refs):
    refs = iter(refs)
    terms, arrived, (dwg, dwu, dwd), (dg, du), outs, swapped, (at_, dyt, mid), held, (to, come) = (
        [next(refs) for _ in name] for name in ("tgu", "rgu", "gud", "gu", "ogu", "sgu", "adm", "hgu", "tc")
    )
    scratch = list(refs)
    i = pl.program_id(0)
    tokens, chunk = h.shape[0], wd.shape[0]
    send, recv, local = scratch[-3:]
    me = Place()
    swap = Swap(me, held, swapped, to, come, chunk)
    phases = reducing(me, Sender(send, recv), terms, arrived, outs, scratch[:-3], local)
    run(phases, WEIGHTS_SLOTS, 0, steps)

    @pl.when(i == 0)
    def _():
        @by_rows(tokens)
        def _(at):
            wide = h[at, :].astype(F32)
            at_[:, at] = (wide * scale_of(wide)).astype(BF16).T
            dyt[:, at] = dy[at, :].T

    wdt = wd[...].T
    for t in range(tokens // tile):
        at = pl.ds(t * tile, tile)
        gg, uu = g[at, :], u[at, :]
        dm = dot(dy[at, :], wdt).astype(BF16).astype(F32)
        sg = jax.nn.sigmoid(gg)
        s = gg * sg
        mid[at, :] = (s * uu).astype(BF16)
        du[at, :] = (dm * s).astype(BF16)
        dg[at, :] = (dm * uu * (sg + s * (1.0 - sg))).astype(BF16)
    dwg[...] = dot(at_[...], dg[...]).astype(BF16)
    dwu[...] = dot(at_[...], du[...]).astype(BF16)
    dwd[...] = dot(dyt[...], mid[...]).T.astype(BF16)
    swap.step(i, steps, dwg, dwu, dwd)
    run(phases, WEIGHTS_SLOTS, 2, steps)


def weights_back(x, dy, wd, g, u, terms, arrived, chunk=256, tile=512):
    _, tokens, d = x.shape
    ff = wd.shape[0]
    whole, across, down, wide = specs(tokens, d, chunk)
    terms = blocks_of(terms)
    out = pl.pallas_call(
        functools.partial(weights_kernel, tile, ff // chunk),
        grid=(ff // chunk,),
        out_shape=[jax.ShapeDtypeStruct((d, ff), BF16)] * 2
        + [jax.ShapeDtypeStruct((ff, d), BF16)]
        + [jax.ShapeDtypeStruct((tokens, ff), BF16)] * 2
        + [jax.ShapeDtypeStruct(t.shape[2:], BF16) for t in terms]
        + swap_shapes(d, ff),
        in_specs=[first_of(tokens, d), whole, down, wide, wide] + [HBM] * 6,
        out_specs=[across, across, down, wide, wide] + [HBM] * 6,
        scratch_shapes=[pltpu.VMEM((d, tokens), BF16)] * 2
        + [pltpu.VMEM((tokens, chunk), BF16)]
        + swap_scratch(d, ff, chunk)
        + reduce_scratch([t.shape for t in terms]),
        compiler_params=pltpu.CompilerParams(collective_id=2, has_side_effects=True, vmem_limit_bytes=67043328),
        name="weights_back",
    )(x, dy, wd, g, u, *terms, *arrived)
    return out[:3], out[3], out[4], out[5:8], out[8:]


INPUT_SLOTS = (0, *(2,) * 3, 6, 10, 12, 14, *(16,) * 4)


def input_kernel(tile, steps, h, dy, wg, wu, dg, du, t0, t1, t2, r0, r1, r2, dx, o0, o1, o2, da, *scratch):
    i, n = pl.program_id(0), pl.num_programs(0)
    tokens = h.shape[0]
    send, recv, local = scratch[-3:]
    phases = reducing(Place(), Sender(send, recv), (t0, t1, t2), (r0, r1, r2), (o0, o1, o2), scratch[:-3], local)
    run(phases, INPUT_SLOTS, 0, steps)

    @pl.when(i == 0)
    def _():
        @by_rows(tokens)
        def _(at):
            da[at, :] = jnp.zeros((256, h.shape[1]), F32)

    wgut = jnp.concatenate([wg[...], wu[...]], 1).T
    for t in range(tokens // tile):
        if t:
            run(phases, INPUT_SLOTS, t, steps)
        at = pl.ds(t * tile, tile)
        da[at, :] += dot(jnp.concatenate([dg[at, :], du[at, :]], 1), wgut)

    @pl.when(i == n - 1)
    def _():
        @by_rows(tokens)
        def _(at):
            dx[at, :] = dh_rows(h, dy, da, at)

    run(phases, INPUT_SLOTS, 2, steps)


def input_back(x, dy, wg, wu, dg, du, terms, arrived, chunk=512, tile=1024):
    _, tokens, d = x.shape
    ff = wg.shape[1]
    whole, across, down, wide = specs(tokens, d, chunk)
    terms = blocks_of(terms)
    out = pl.pallas_call(
        functools.partial(input_kernel, tile, ff // chunk),
        grid=(ff // chunk,),
        out_shape=[jax.ShapeDtypeStruct(x.shape, BF16)] + [jax.ShapeDtypeStruct(t.shape[2:], BF16) for t in terms],
        in_specs=[first_of(tokens, d), whole, across, across, wide, wide] + [HBM] * 6,
        out_specs=[first_of(tokens, d)] + [HBM] * 3,
        scratch_shapes=[pltpu.VMEM((tokens, d), F32)] + reduce_scratch([t.shape for t in terms]),
        compiler_params=pltpu.CompilerParams(collective_id=3, has_side_effects=True, vmem_limit_bytes=67043328),
        name="input_back",
    )(x, dy, wg, wu, dg, du, *terms, *arrived)
    return out[0], out[1:]


def solution(mesh):
    def step(x, dy, *weights):
        w0 = gathered(weights, 0)
        g0, u0, h1, w1 = forward(x, w0, weights, 1)
        terms1, by_h, arrived1 = backward(h1, dy, w1)
        terms0, dg, du, mine1, arrived0 = weights_back(x, by_h, w0[2], g0, u0, terms1, arrived1)
        by_x, mine0 = input_back(x, by_h, w0[0], w0[1], dg, du, terms0, arrived0)
        return (by_x, *(jnp.stack([a, b]) for a, b in zip(mine0, mine1)))

    states, cut = P(("rep", "r", "s"), None, None), P(None, "s", None)
    return jax.shard_map(
        step,
        mesh=mesh,
        in_specs=(states, states) + (cut,) * 3,
        out_specs=(states,) + (P("rep", "s", None),) * 3,
        check_vma=False,
    )
```
